256 devices in a mesh: group: 8 (over x, core), dev: 32 (over z, y).
Axes of the slice: x: 4, y: 4, z: 8, core: 2. Of those that a mesh axis runs over, the one named last changes fastest.
Arguments:
- state: float32 [5, 4, 4, 4, 16, 64, 128], P(None, None, None, None, 'group', 'dev'), may hold values from -3 to 19.25, as said below
- limit_slot: int32 [16, 64, 128], P('group', 'dev'), may hold values from -1 to 511, as said below
- wall_owner: int32 [16, 64, 2], P('group', 'dev'), may hold values from 0 to 2047
Outputs:
- state_next: float32 [5, 4, 4, 4, 16, 64, 128], P(None, None, None, None, 'group', 'dev')
- wall_loads: float32 [2048], P(('group', 'dev'))
The draws below stay inside these ranges and needn't reach their ends.
Inputs may be any that keep to these rules, and one draw needn't show every extreme that they name: `state`: density lies in 0.5 to 2, each velocity component in -1.5 to 1.5 and p in 0.2 to 5 at every node. A troubled element has limit_slot = destination * 16 + slot, the destination an index of dev within the element's group and the slot below 16. The troubled elements of one device have distinct values and fill whole blocks of 16 slots per destination; one device has at most 512 troubled elements, some device of every group has exactly 512, and every device is the destination of exactly 128 troubled elements of its group.
All inputs are finite; a program needn't handle non-finite values.
Results may differ from the reference program's by a relative error of at most 0.00013.
Values sent between devices are 32-bit elements; how exact they have to be, the bound alone decides.
No kernel may reach another device: no remote copies, remote signals or barrier semaphores. Data moves between devices by JAX's collectives and lax.ppermute only.
A program may use at most 64 MiB of HBM per device.

```python
import jax
import jax.numpy as jnp
import numpy as np
from jax import lax

SUBSTEPS = 8
EX = 2
EY = 2
NZ = 128
CAP = 16
NX = 16
NY = 64
SNODES = 2048


def draw_state(key, part):
    keys = jax.random.split(key, 3)
    field_shape = (4, 4, 4, NX, NY, NZ)
    density = jnp.exp(jax.random.uniform(keys[0], field_shape, jnp.float32, jnp.log(0.5), jnp.log(2.0)))
    velocity = jnp.clip(0.5 * jax.random.normal(keys[1], (3,) + field_shape, jnp.float32), -1.5, 1.5)
    pressure = jnp.exp(jax.random.uniform(keys[2], field_shape, jnp.float32, jnp.log(0.2), jnp.log(5.0)))
    kinetic = 0.5 * density * (velocity[0] * velocity[0] + velocity[1] * velocity[1] + velocity[2] * velocity[2])
    energy = pressure / 0.4 + kinetic
    return jnp.stack([density, density * velocity[0], density * velocity[1], density * velocity[2], energy]).astype(jnp.float32)


def draw_limit_slot(key, part):
    n_group = NX // EX
    n_dev = NY // EY
    per_device = EX * EY * NZ
    blocks_of = jnp.where(jnp.arange(n_dev, dtype=jnp.int32) < n_dev // 4, n_dev, 0).astype(jnp.int32)

    def one_group(group_key):
        order_key, offset_key, rank_key = jax.random.split(group_key, 3)
        source_order = jax.random.permutation(order_key, n_dev)
        starts = jax.random.randint(offset_key, (n_dev,), 0, n_dev)
        position = jnp.zeros(n_dev, jnp.int32).at[source_order].set(jnp.arange(n_dev, dtype=jnp.int32))
        source_blocks = blocks_of[position]
        source_start = starts[position]
        element_rank = jax.vmap(lambda device_key: jax.random.permutation(device_key, per_device))(jax.random.split(rank_key, n_dev))
        troubled = element_rank < source_blocks[:, None] * CAP
        destination = (source_start[:, None] + element_rank // CAP) % n_dev
        return jnp.where(troubled, destination * CAP + element_rank % CAP, -1)
    values = jax.vmap(one_group)(jax.random.split(key, n_group))
    values = values.reshape(n_group, n_dev, EX, EY, NZ).transpose(0, 2, 1, 3, 4).reshape(NX, NY, NZ)
    return values.astype(jnp.int32)


def set_ends(result, stream_key, low, top_value):
    longest = result.shape.index(max(result.shape))
    spots = []
    for shift in (0, 1):
        where = [jax.random.randint(jax.random.fold_in(stream_key, axis), (), 0, length) for axis, length in enumerate(result.shape)]
        where[longest] = (where[longest] + shift) % result.shape[longest]
        spots.append(tuple(where))
    return result.at[spots[0]].set(low).at[spots[1]].set(top_value)


def setup_inputs(seed: int = 0) -> dict:
    arg_keys = jax.random.split(jax.random.key(seed), 4)
    state = draw_state(jax.random.fold_in(arg_keys[3], 71), 0)
    limit_slot = draw_limit_slot(jax.random.fold_in(arg_keys[3], 71), 0)
    wall_owner = set_ends(jax.random.randint(arg_keys[2], (NX, NY, 2), 0, SNODES), jax.random.fold_in(arg_keys[2], 1), 0, SNODES - 1).astype(jnp.int32)
    return dict(state=state, limit_slot=limit_slot, wall_owner=wall_owner)


gamma_ratio = 1.4
courant = 0.02

def gll_tables():
    gll_nodes = np.array([-1.0, -np.sqrt(0.2), np.sqrt(0.2), 1.0])
    weights = np.array([1.0, 5.0, 5.0, 1.0]) / 6.0
    bary_weights = np.array([1.0 / np.prod([gll_nodes[index_a] - gll_nodes[index_b] for index_b in range(4) if index_b != index_a]) for index_a in range(4)])
    derivative = np.zeros((4, 4))
    for index_a in range(4):
        for index_b in range(4):
            if index_a != index_b:
                derivative[index_a, index_b] = bary_weights[index_b] / bary_weights[index_a] / (gll_nodes[index_a] - gll_nodes[index_b])
        derivative[index_a, index_a] = -np.sum(derivative[index_a])
    return (jnp.asarray(derivative, jnp.float32), jnp.asarray(weights, jnp.float32))

def euler_flux(conserved, direction):
    density = conserved[0]
    normal_velocity = conserved[1 + direction] / density
    pressure = (gamma_ratio - 1.0) * (conserved[4] - 0.5 * (conserved[1] * conserved[1] + conserved[2] * conserved[2] + conserved[3] * conserved[3]) / density)
    flux_rows = [conserved[1 + direction]]
    for component in range(3):
        momentum_flux = conserved[1 + component] * normal_velocity
        if component == direction:
            momentum_flux = momentum_flux + pressure
        flux_rows.append(momentum_flux)
    flux_rows.append(normal_velocity * (conserved[4] + pressure))
    wave_speed = jnp.abs(normal_velocity) + jnp.sqrt(gamma_ratio * pressure / density)
    return (jnp.stack(flux_rows), wave_speed)

def rusanov(left_state, right_state, direction):
    left_flux, left_speed = euler_flux(left_state, direction)
    right_flux, right_speed = euler_flux(right_state, direction)
    fastest = jnp.maximum(left_speed, right_speed)
    return 0.5 * (left_flux + right_flux) - 0.5 * fastest * (right_state - left_state)

def mirrored(conserved):
    return jnp.concatenate([conserved[:3], -conserved[3:4], conserved[4:]], axis=0)

def node_index(node_axis, which):
    return (slice(None),) * node_axis + (which,)

def dg_rate(state, direction, flux_low, flux_high, derivative, weights):
    node_flux, wave_speed = euler_flux(state, direction)
    einsum_forms = ['ai,vijk...->vajk...', 'aj,vijk...->viak...', 'ak,vijk...->vija...']
    volume = jnp.einsum(einsum_forms[direction], derivative, node_flux, precision=lax.Precision.HIGHEST)
    node_axis = 1 + direction
    low_index = node_index(node_axis, 0)
    high_index = node_index(node_axis, 3)
    volume = volume.at[low_index].add(-(flux_low - node_flux[low_index]) / weights[0])
    volume = volume.at[high_index].add((flux_high - node_flux[high_index]) / weights[3])
    return volume

def fv_rate(state, direction, flux_low, flux_high, weights):
    node_axis = 1 + direction
    lower_nodes = lax.slice_in_dim(state, 0, 3, axis=node_axis)
    upper_nodes = lax.slice_in_dim(state, 1, 4, axis=node_axis)
    inner_flux = rusanov(lower_nodes, upper_nodes, direction)
    interfaces = jnp.concatenate([jnp.expand_dims(flux_low, node_axis), inner_flux, jnp.expand_dims(flux_high, node_axis)], axis=node_axis)
    width_shape = [1] * state.ndim
    width_shape[node_axis] = 4
    widths = weights.reshape(width_shape)
    upper_faces = lax.slice_in_dim(interfaces, 1, 5, axis=node_axis)
    lower_faces = lax.slice_in_dim(interfaces, 0, 4, axis=node_axis)
    return (upper_faces - lower_faces) / widths

def dg_next(state, fluxes, derivative, weights):
    rate_sum = dg_rate(state, 0, fluxes[0], fluxes[1], derivative, weights)
    rate_sum = rate_sum + dg_rate(state, 1, fluxes[2], fluxes[3], derivative, weights)
    rate_sum = rate_sum + dg_rate(state, 2, fluxes[4], fluxes[5], derivative, weights)
    return state - courant * rate_sum

def fv_next(state, fluxes, weights):
    sub_state = state
    for substep in range(SUBSTEPS):
        rate_sum = fv_rate(sub_state, 0, fluxes[0], fluxes[1], weights)
        rate_sum = rate_sum + fv_rate(sub_state, 1, fluxes[2], fluxes[3], weights)
        rate_sum = rate_sum + fv_rate(sub_state, 2, fluxes[4], fluxes[5], weights)
        sub_state = sub_state - courant / SUBSTEPS * rate_sum
    return sub_state

def z_fluxes(state):
    z_low, z_high = (state[:, :, :, 0], state[:, :, :, 3])
    below_states = jnp.concatenate([mirrored(z_low[..., 0:1]), z_high[..., :-1]], axis=-1)
    z_flux_low = rusanov(below_states, z_low, 2)
    top_flux = rusanov(z_high[..., -1:], mirrored(z_high[..., -1:]), 2)
    z_flux_high = jnp.concatenate([z_flux_low[..., 1:], top_flux], axis=-1)
    return (z_flux_low, z_flux_high, top_flux)

def wall_face_loads(z_flux_low, top_flux, weights):
    face_weights = weights[:, None] * weights[None, :]
    bottom_load = -lax.optimization_barrier(jnp.sum(face_weights[:, :, None, None] * z_flux_low[3, :, :, :, :, 0], axis=(0, 1)))
    top_load = lax.optimization_barrier(jnp.sum(face_weights[:, :, None, None] * top_flux[3, :, :, :, :, 0], axis=(0, 1)))
    return jnp.stack([bottom_load, top_load], axis=-1)

def reference(state, limit_slot, wall_owner):
    derivative, weights = gll_tables()
    x_low, x_high = (state[:, 0], state[:, 3])
    x_flux_low = rusanov(jnp.roll(x_high, 1, axis=3), x_low, 0)
    x_flux_high = jnp.roll(x_flux_low, -1, axis=3)
    y_low, y_high = (state[:, :, 0], state[:, :, 3])
    y_flux_low = rusanov(jnp.roll(y_high, 1, axis=4), y_low, 1)
    y_flux_high = jnp.roll(y_flux_low, -1, axis=4)
    z_flux_low, z_flux_high, top_flux = z_fluxes(state)
    fluxes = [x_flux_low, x_flux_high, y_flux_low, y_flux_high, z_flux_low, z_flux_high]
    dg_state = dg_next(state, fluxes, derivative, weights)
    fv_state = fv_next(state, fluxes, weights)
    state_next = jnp.where(limit_slot >= 0, fv_state, dg_state)
    face_load = wall_face_loads(z_flux_low, top_flux, weights)
    wall_loads = jax.ops.segment_sum(face_load.reshape(-1), wall_owner.reshape(-1).astype(jnp.int32), num_segments=SNODES)
    return (state_next, wall_loads)
```

```python
import jax
import jax.numpy as jnp
import numpy as np
from jax import lax
from jax.experimental import pallas as pl
from jax.experimental.pallas import tpu as pltpu
from jax.sharding import PartitionSpec as P

SUBSTEPS = 8
SN_DEV = 8
GAMMA = 1.4
COURANT = 0.02
F32 = jnp.float32

ROWS = 1280


def blk(v, i, j, h):
    return (((v * 4 + i) * 4 + j) * 2 + h) * 8


def nod(q, i, j, h):
    return q * 256 + ((i * 4 + j) * 2 + h) * 8


FLUX_OF = (
    (None, 0, 1, 2, 6),
    (None, 1, 3, 4, 7),
    (None, 2, 4, 5, 8),
)


def derivative_table():
    gll_nodes = np.array([-1.0, -np.sqrt(0.2), np.sqrt(0.2), 1.0])
    bary = np.array(
        [1.0 / np.prod([gll_nodes[a] - gll_nodes[b] for b in range(4) if b != a]) for a in range(4)]
    )
    table = np.zeros((4, 4))
    for a in range(4):
        for b in range(4):
            if a != b:
                table[a, b] = bary[b] / bary[a] / (gll_nodes[a] - gll_nodes[b])
    for a in (0, 3):
        table[a, a] = -np.sum(table[a])
    return table


WEIGHTS = np.array([1.0, 5.0, 5.0, 1.0]) / 6.0


def row_bit(bit):
    rows = lax.broadcasted_iota(jnp.int32, (8, 128), 0)
    return (rows & bit) != 0


def turn(x, shift):
    return pltpu.roll(x, shift % 8, 0)


def point_flux(u, d):
    inv = 1.0 / u[0]
    v = u[1 + d] * inv
    ke = (u[1] * u[1] + u[2] * u[2] + u[3] * u[3]) * inv
    p = (GAMMA - 1.0) * (u[4] - 0.5 * ke)
    flux = [u[1 + d]] + [u[1 + a] * v for a in range(3)] + [v * (u[4] + p)]
    flux[1 + d] = flux[1 + d] + p
    speed = jnp.abs(v) + jnp.sqrt(GAMMA * p * inv)
    return flux, speed


def twice_face(fl, fr, s, ul, ur):
    return (fl + fr) - s * (ur - ul)


def z_wall_pair(own, lane):
    low = jnp.logical_not(row_bit(4))
    wall = (low & (lane == 0)) | (row_bit(4) & (lane == 127))
    across = []
    for c in range(5):
        x = turn(own[c], 4)
        n = jnp.where(low, pltpu.roll(x, 1, 1), pltpu.roll(x, 127, 1))
        across.append(jnp.where(wall, -own[c] if c == 3 else own[c], n))
    return across


def prepare_kernel(s_ref, own_ref, xl_ref, xh_ref, yl_ref, yh_ref, part_ref):
    bx, by, bk = row_bit(2), row_bit(1), row_bit(4)
    lane = lax.broadcasted_iota(jnp.int32, (8, 128), 1)

    def get(v, i, j, h):
        return s_ref[pl.ds(blk(v, i, j, h), 8), :]

    for c in range(5):
        for a in range(4):
            row = pl.ds((c * 4 + a) * 8, 8)
            xl_ref[row, :] = jnp.where(bx, get(c, 3, a, 1), turn(get(c, 3, a, 0), -2))
            xh_ref[row, :] = jnp.where(bx, turn(get(c, 0, a, 0), 2), get(c, 0, a, 1))
            yl_ref[row, :] = jnp.where(by, get(c, a, 3, 1), turn(get(c, a, 3, 0), -1))
            yh_ref[row, :] = jnp.where(by, turn(get(c, a, 0, 0), 1), get(c, a, 0, 1))

    total = jnp.zeros((8, 128), F32)
    sign = jnp.where(bk, 0.5, -0.5).astype(F32)
    for i in range(4):
        for j in range(4):
            own = [jnp.where(bk, get(c, i, j, 1), get(c, i, j, 0)) for c in range(5)]
            across = list(own)
            across[3] = -own[3]
            fo, so = point_flux(own, 2)
            fa, sa = point_flux(across, 2)
            jump = jnp.where(bk, across[3] - own[3], own[3] - across[3])
            flux = (fo[3] + fa[3]) - jnp.maximum(so, sa) * jump
            total = total + float(WEIGHTS[i] * WEIGHTS[j]) * flux
    at_wall = (bk & (lane == 127)) | (jnp.logical_not(bk) & (lane == 0))
    loads = jnp.sum(jnp.where(at_wall, total * sign, 0.0), axis=1, keepdims=True)
    part_ref[...] = jnp.zeros(part_ref.shape, F32)
    lane1 = lax.broadcasted_iota(jnp.int32, (1, 128), 1)
    for side in range(2):
        for x in range(2):
            for y in range(2):
                node = own_ref[x, y, side]
                r = side * 4 + x * 2 + y
                at = pl.ds(node // SN_DEV, 1)
                part_ref[at, :] = part_ref[at, :] + jnp.where(
                    lane1 == node % SN_DEV, loads[r : r + 1, :], 0.0
                )


def section_kernel(
    s_ref, slot_ref, xl_ref, xh_ref, yl_ref, yh_ref, out_ref,
    u_ref, f_ref, s3_ref, sm_ref, gx_ref, gy_ref, gz_ref,
):
    bx, by, bk = row_bit(2), row_bit(1), row_bit(4)
    low = jnp.logical_not(bk)
    lane = lax.broadcasted_iota(jnp.int32, (8, 128), 1)
    IJ = [(i, j) for i in range(4) for j in range(4)]

    def nodal(src):
        for i, j in IJ:
            for h in range(2):
                u = [src[pl.ds(blk(c, i, j, h), 8), :] for c in range(5)]
                inv = 1.0 / u[0]
                v = [u[1 + d] * inv for d in range(3)]
                xx, xy, xz = u[1] * v[0], u[1] * v[1], u[1] * v[2]
                yy, yz, zz = u[2] * v[1], u[2] * v[2], u[3] * v[2]
                p = (GAMMA - 1.0) * (u[4] - 0.5 * (xx + yy + zz))
                e = u[4] + p
                sound = jnp.sqrt(GAMMA * p * inv)
                q = [xx + p, xy, xz, yy + p, yz, zz + p, v[0] * e, v[1] * e, v[2] * e]
                for n in range(9):
                    f_ref[pl.ds(nod(n, i, j, h), 8), :] = q[n]
                for d in range(3):
                    s3_ref[pl.ds(nod(d, i, j, h), 8), :] = jnp.abs(v[d]) + sound
        for a in range(3):
            for b in range(4):
                for h in range(2):
                    sm_ref[pl.ds(nod(0, a, b, h), 8), :] = jnp.maximum(
                        s3_ref[pl.ds(nod(0, a, b, h), 8), :], s3_ref[pl.ds(nod(0, a + 1, b, h), 8), :]
                    )
                    sm_ref[pl.ds(nod(1, b, a, h), 8), :] = jnp.maximum(
                        s3_ref[pl.ds(nod(1, b, a, h), 8), :], s3_ref[pl.ds(nod(1, b, a + 1, h), 8), :]
                    )
        for i, j in IJ:
            mid = s3_ref[pl.ds(nod(2, i, j, 0) + 4, 8), :]
            for h in range(2):
                sm_ref[pl.ds(nod(2, i, j, h), 8), :] = jnp.maximum(
                    s3_ref[pl.ds(nod(2, i, j, h), 8), :], mid
                )

    def flux(src, d, c, i, j, h, off=0):
        if c == 0:
            return src[pl.ds(blk(1 + d, i, j, h) + off, 8), :]
        return f_ref[pl.ds(nod(FLUX_OF[d][c], i, j, h) + off, 8), :]

    def cell(src, c, i, j, h, off=0):
        return src[pl.ds(blk(c, i, j, h) + off, 8), :]

    nodal(s_ref)
    for b in range(4):
        for h in range(2):
            for d, g_ref, lo_ref, hi_ref, bit, step in (
                (0, gx_ref, xl_ref, xh_ref, bx, 2),
                (1, gy_ref, yl_ref, yh_ref, by, 1),
            ):
                first = (0, b) if d == 0 else (b, 0)
                last = (3, b) if d == 0 else (b, 3)
                uf = [cell(s_ref, c, *first, h) for c in range(5)]
                ul = [cell(s_ref, c, *last, h) for c in range(5)]
                hl = [lo_ref[pl.ds((c * 4 + b) * 8, 8), :] for c in range(5)]
                hh = [hi_ref[pl.ds((c * 4 + b) * 8, 8), :] for c in range(5)]
                if h == 1:
                    hl = [turn(t, -step) for t in hl]
                    hh = [turn(t, step) for t in hh]
                before = [jnp.where(bit, turn(ul[c], step), hl[c]) for c in range(5)]
                after = [jnp.where(bit, hh[c], turn(uf[c], -step)) for c in range(5)]
                fb, sb = point_flux(before, d)
                fa, sa = point_flux(after, d)
                sl = jnp.maximum(sb, s3_ref[pl.ds(nod(d, *first, h), 8), :])
                sh = jnp.maximum(sa, s3_ref[pl.ds(nod(d, *last, h), 8), :])
                for c in range(5):
                    at = ((c * 4 + b) * 2 + h) * 8
                    g_ref[pl.ds(at, 8), :] = twice_face(
                        fb[c], flux(s_ref, d, c, *first, h), sl, before[c], uf[c]
                    )
                    g_ref[pl.ds(320 + at, 8), :] = twice_face(
                        flux(s_ref, d, c, *last, h), fa[c], sh, ul[c], after[c]
                    )
    for i, j in IJ:
        own = [jnp.where(bk, cell(s_ref, c, i, j, 1), cell(s_ref, c, i, j, 0)) for c in range(5)]
        across = z_wall_pair(own, lane)
        fo, so = point_flux(own, 2)
        fa, sa = point_flux(across, 2)
        s = jnp.maximum(so, sa)
        s = jnp.where(bk, s, -s)
        for c in range(5):
            gz_ref[pl.ds(((c * 4 + i) * 4 + j) * 8, 8), :] = (fo[c] + fa[c]) - s * (across[c] - own[c])

    def gxy(g_ref, side, c, b, h):
        return g_ref[pl.ds(side * 320 + ((c * 4 + b) * 2 + h) * 8, 8), :]

    def gz(c, i, j):
        return gz_ref[pl.ds(((c * 4 + i) * 4 + j) * 8, 8), :]

    table = derivative_table()
    table[0, 0] += 1.0 / WEIGHTS[0]
    table[3, 3] -= 1.0 / WEIGHTS[3]
    table = COURANT * table
    lift = COURANT * 0.5 / WEIGHTS[0]

    def lanes_pair(lo_value, hi_value):
        return jnp.where(bk, float(hi_value), float(lo_value)).astype(F32)

    zc = [
        [lanes_pair(table[2 * h, 2 * g], table[2 * h + 1, 2 * g + 1]) for g in range(2)]
        + [lanes_pair(table[2 * h, 2 * g + 1], table[2 * h + 1, 2 * g]) for g in range(2)]
        for h in range(2)
    ]
    zl = [lanes_pair(-lift, 0.0), lanes_pair(0.0, lift)]

    for c in range(5):
        for h in range(2):
            acc = {}
            for b in range(4):
                for d in range(2):
                    line = [(a, b) if d == 0 else (b, a) for a in range(4)]
                    fl = [flux(s_ref, d, c, *n, h) for n in line]
                    g_ref = gx_ref if d == 0 else gy_ref
                    for a in range(4):
                        r = None
                        for m in range(4):
                            if table[a, m] != 0.0:
                                t = float(table[a, m]) * fl[m]
                                r = t if r is None else r + t
                        if a == 0:
                            r = r - float(lift) * gxy(g_ref, 0, c, b, h)
                        if a == 3:
                            r = r + float(lift) * gxy(g_ref, 1, c, b, h)
                        acc.setdefault(line[a], []).append(r)
            for i, j in IJ:
                fa = flux(s_ref, 2, c, i, j, 0)
                fb = flux(s_ref, 2, c, i, j, 1)
                r = zc[h][0] * fa + zc[h][1] * fb + zc[h][2] * turn(fa, 4) + zc[h][3] * turn(fb, 4)
                r = r + zl[h] * gz(c, i, j)
                r = r + (acc[i, j][0] + acc[i, j][1])
                out_ref[pl.ds(blk(c, i, j, h), 8), :] = cell(s_ref, c, i, j, h) - r

    scale = COURANT / SUBSTEPS * 0.5 / WEIGHTS
    kz = [lanes_pair(scale[0], scale[1]), lanes_pair(scale[2], scale[3])]

    def advance(src, put):
        for c in range(5):
            done = {}
            for h in range(2):
                diff = {}
                for b in range(4):
                    for d in range(2):
                        line = [(a, b) if d == 0 else (b, a) for a in range(4)]
                        g_ref = gx_ref if d == 0 else gy_ref
                        u = [cell(src, c, *n, h) for n in line]
                        f = [flux(src, d, c, *n, h) for n in line]
                        g = [gxy(g_ref, 0, c, b, h)]
                        for a in range(3):
                            g.append(
                                twice_face(
                                    f[a], f[a + 1],
                                    sm_ref[pl.ds(nod(d, *line[a], h), 8), :],
                                    u[a], u[a + 1],
                                )
                            )
                        g.append(gxy(g_ref, 1, c, b, h))
                        for a in range(4):
                            diff[d, line[a]] = g[a + 1] - g[a]
                for i, j in IJ:
                    if scale[i] == scale[j]:
                        r = float(scale[i]) * (diff[0, (i, j)] + diff[1, (i, j)])
                    else:
                        r = float(scale[i]) * diff[0, (i, j)] + float(scale[j]) * diff[1, (i, j)]
                    u = cell(src, c, i, j, h)
                    um = cell(src, c, i, j, 0, 4)
                    fz = flux(src, 2, c, i, j, h)
                    fm = flux(src, 2, c, i, j, 0, 4)
                    s = sm_ref[pl.ds(nod(2, i, j, h), 8), :]
                    if h == 0:
                        t = twice_face(fz, fm, s, u, um)
                        dz = t - jnp.where(low, gz(c, i, j), turn(t, 4))
                    else:
                        t = twice_face(fm, fz, s, um, u)
                        dz = jnp.where(low, turn(t, 4), gz(c, i, j)) - t
                    done[i, j, h] = u - (r + kz[h] * dz)
            for (i, j, h), value in done.items():
                put(c, i, j, h, value)

    def put_u(c, i, j, h, value):
        u_ref[pl.ds(blk(c, i, j, h), 8), :] = value

    def put_out(c, i, j, h, value):
        at = pl.ds(blk(c, i, j, h), 8)
        out_ref[at, :] = jnp.where(troubled, value, out_ref[at, :])

    u_ref[...] = s_ref[...]

    def substep(_, carry):
        advance(u_ref, put_u)
        nodal(u_ref)
        return carry

    lax.fori_loop(0, SUBSTEPS - 1, substep, 0)
    slot = slot_ref[...]
    troubled = jnp.concatenate([slot, slot], axis=0) >= 0
    advance(u_ref, put_out)


def on_device(state, limit_slot, wall_owner, interpret=False):
    n_group, n_dev = lax.axis_size("group"), lax.axis_size("dev")
    devices = n_group * n_dev
    rows = state.reshape(ROWS, 128)
    halo = jax.ShapeDtypeStruct((160, 128), F32)
    vmem = pl.BlockSpec(memory_space=pltpu.VMEM)
    xl, xh, yl, yh, part = pl.pallas_call(
        prepare_kernel,
        out_shape=(halo, halo, halo, halo, jax.ShapeDtypeStruct((devices, 128), F32)),
        in_specs=[vmem, pl.BlockSpec(memory_space=pltpu.SMEM)],
        out_specs=(vmem,) * 5,
        name="prepare",
        interpret=interpret,
    )(rows, wall_owner)

    def shift(x, axis, by):
        n = lax.axis_size(axis)
        return lax.ppermute(x, axis, [(i, (i + by) % n) for i in range(n)])

    xl, xh = shift(xl, "group", 1), shift(xh, "group", -1)
    yl, yh = shift(yl, "dev", 1), shift(yh, "dev", -1)
    parts = lax.all_to_all(part, ("group", "dev"), 0, 0, tiled=True)
    wall_loads = jnp.sum(parts[:, :SN_DEV], axis=0)
    out = pl.pallas_call(
        section_kernel,
        out_shape=jax.ShapeDtypeStruct((ROWS, 128), F32),
        in_specs=[vmem] * 6,
        out_specs=vmem,
        scratch_shapes=[
            pltpu.VMEM((ROWS, 128), F32),
            pltpu.VMEM((9 * 256, 128), F32),
            pltpu.VMEM((3 * 256, 128), F32),
            pltpu.VMEM((3 * 256, 128), F32),
            pltpu.VMEM((640, 128), F32),
            pltpu.VMEM((640, 128), F32),
            pltpu.VMEM((640, 128), F32),
        ],
        cost_estimate=pl.CostEstimate(flops=60_000_000, transcendentals=600_000, bytes_accessed=2_000_000),
        name="section",
        interpret=interpret,
    )(rows, limit_slot.reshape(4, 128), xl, xh, yl, yh)
    return out.reshape(state.shape), wall_loads


def solution(mesh):
    in_specs = (
        P(None, None, None, None, "group", "dev", None),
        P("group", "dev", None),
        P("group", "dev", None),
    )
    out_specs = (P(None, None, None, None, "group", "dev", None), P(("group", "dev")))
    return jax.shard_map(
        on_device, mesh=mesh, in_specs=in_specs, out_specs=out_specs, check_vma=False
    )
```

```python
import jax
import jax.numpy as jnp
import numpy as np
from jax import lax
from jax.experimental import pallas as pl
from jax.experimental.pallas import tpu as pltpu
from jax.sharding import PartitionSpec as P


SUBSTEPS = 8
SN_DEV = 8
GAMMA = 1.4
COURANT = 0.02
F32 = jnp.float32

ROWS = 1280
VMEM_LIMIT = 16 * 1024 * 1024


def blk(v, i, j, h):
    return (((v * 4 + i) * 4 + j) * 2 + h) * 8


def nod(q, i, j, h):
    return q * 256 + ((i * 4 + j) * 2 + h) * 8


FLUX_OF = (
    (None, 0, 1, 2, 6),
    (None, 1, 3, 4, 7),
    (None, 2, 4, 5, 8),
)


def derivative_table():
    gll_nodes = np.array([-1.0, -np.sqrt(0.2), np.sqrt(0.2), 1.0])
    bary = np.array(
        [1.0 / np.prod([gll_nodes[a] - gll_nodes[b] for b in range(4) if b != a]) for a in range(4)]
    )
    table = np.zeros((4, 4))
    for a in range(4):
        for b in range(4):
            if a != b:
                table[a, b] = bary[b] / bary[a] / (gll_nodes[a] - gll_nodes[b])
    for a in (0, 3):
        table[a, a] = -np.sum(table[a])
    return table


WEIGHTS = np.array([1.0, 5.0, 5.0, 1.0]) / 6.0


def row_bit(bit):
    rows = lax.broadcasted_iota(jnp.int32, (8, 128), 0)
    return (rows & bit) != 0


def turn(x, shift):
    return pltpu.roll(x, shift % 8, 0)


def point_flux(u, d):
    inv = 1.0 / u[0]
    v = u[1 + d] * inv
    ke = (u[1] * u[1] + u[2] * u[2] + u[3] * u[3]) * inv
    p = (GAMMA - 1.0) * (u[4] - 0.5 * ke)
    flux = [u[1 + d]] + [u[1 + a] * v for a in range(3)] + [v * (u[4] + p)]
    flux[1 + d] = flux[1 + d] + p
    speed = jnp.abs(v) + jnp.sqrt(GAMMA * p * inv)
    return flux, speed


def twice_face(fl, fr, s, ul, ur):
    return (fl + fr) - s * (ur - ul)


def z_wall_pair(own, lane):
    low = jnp.logical_not(row_bit(4))
    wall = (low & (lane == 0)) | (row_bit(4) & (lane == 127))
    across = []
    for c in range(5):
        x = turn(own[c], 4)
        n = jnp.where(low, pltpu.roll(x, 1, 1), pltpu.roll(x, 127, 1))
        across.append(jnp.where(wall, -own[c] if c == 3 else own[c], n))
    return across


def parity(axis):
    return jnp.full((8, 128), lax.axis_index(axis) % 2, jnp.int32) == 0


def prepare_kernel(s_ref, own_ref, ye_ref, yo_ref, xe_ref, xo_ref, part_ref):
    bx, by, bk = row_bit(2), row_bit(1), row_bit(4)
    lane = lax.broadcasted_iota(jnp.int32, (8, 128), 1)

    def get(v, i, j, h):
        return s_ref[pl.ds(blk(v, i, j, h), 8), :]

    ex, ey = parity("group"), parity("dev")
    for c in range(5):
        for a in range(4):
            row = pl.ds((c * 4 + a) * 8, 8)
            top = jnp.where(by, get(c, a, 3, 1), turn(get(c, a, 3, 0), -1))
            low = jnp.where(by, turn(get(c, a, 0, 0), 1), get(c, a, 0, 1))
            ye_ref[row, :] = jnp.where(ey, top, low)
            yo_ref[row, :] = jnp.where(ey, low, top)
            top = jnp.where(bx, get(c, 3, a, 1), turn(get(c, 3, a, 0), -2))
            low = jnp.where(bx, turn(get(c, 0, a, 0), 2), get(c, 0, a, 1))
            xe_ref[row, :] = jnp.where(ex, top, low)
            xo_ref[row, :] = jnp.where(ex, low, top)

    total = jnp.zeros((8, 128), F32)
    sign = jnp.where(bk, 0.5, -0.5).astype(F32)
    for i in range(4):
        for j in range(4):
            own = [jnp.where(bk, get(c, i, j, 1), get(c, i, j, 0)) for c in range(5)]
            across = list(own)
            across[3] = -own[3]
            fo, so = point_flux(own, 2)
            fa, sa = point_flux(across, 2)
            jump = jnp.where(bk, across[3] - own[3], own[3] - across[3])
            flux = (fo[3] + fa[3]) - jnp.maximum(so, sa) * jump
            total = total + float(WEIGHTS[i] * WEIGHTS[j]) * flux
    at_wall = (bk & (lane == 127)) | (jnp.logical_not(bk) & (lane == 0))
    loads = jnp.sum(jnp.where(at_wall, total * sign, 0.0), axis=1, keepdims=True)
    part_ref[...] = jnp.zeros(part_ref.shape, F32)
    lane1 = lax.broadcasted_iota(jnp.int32, (1, SN_DEV), 1)
    for side in range(2):
        for x in range(2):
            for y in range(2):
                node = own_ref[x, y, side]
                r = side * 4 + x * 2 + y
                at = pl.ds(node // SN_DEV, 1)
                part_ref[at, :] = part_ref[at, :] + jnp.where(
                    lane1 == node % SN_DEV, loads[r : r + 1, :], 0.0
                )


def section_kernel(
    s_ref, slot_ref, ye_ref, yo_ref, xe_ref, xo_ref, out_ref,
    u_ref, f_ref, s3_ref, sm_ref, gx_ref, gy_ref, gz_ref,
):
    bx, by, bk = row_bit(2), row_bit(1), row_bit(4)
    low = jnp.logical_not(bk)
    lane = lax.broadcasted_iota(jnp.int32, (8, 128), 1)
    IJ = [(i, j) for i in range(4) for j in range(4)]

    def nodal(src):
        for i, j in IJ:
            for h in range(2):
                u = [src[pl.ds(blk(c, i, j, h), 8), :] for c in range(5)]
                inv = 1.0 / u[0]
                v = [u[1 + d] * inv for d in range(3)]
                xx, xy, xz = u[1] * v[0], u[1] * v[1], u[1] * v[2]
                yy, yz, zz = u[2] * v[1], u[2] * v[2], u[3] * v[2]
                p = (GAMMA - 1.0) * (u[4] - 0.5 * (xx + yy + zz))
                e = u[4] + p
                sound = jnp.sqrt(GAMMA * p * inv)
                q = [xx + p, xy, xz, yy + p, yz, zz + p, v[0] * e, v[1] * e, v[2] * e]
                for n in range(9):
                    f_ref[pl.ds(nod(n, i, j, h), 8), :] = q[n]
                for d in range(3):
                    s3_ref[pl.ds(nod(d, i, j, h), 8), :] = jnp.abs(v[d]) + sound
        for a in range(3):
            for b in range(4):
                for h in range(2):
                    sm_ref[pl.ds(nod(0, a, b, h), 8), :] = jnp.maximum(
                        s3_ref[pl.ds(nod(0, a, b, h), 8), :], s3_ref[pl.ds(nod(0, a + 1, b, h), 8), :]
                    )
                    sm_ref[pl.ds(nod(1, b, a, h), 8), :] = jnp.maximum(
                        s3_ref[pl.ds(nod(1, b, a, h), 8), :], s3_ref[pl.ds(nod(1, b, a + 1, h), 8), :]
                    )
        for i, j in IJ:
            mid = s3_ref[pl.ds(nod(2, i, j, 0) + 4, 8), :]
            for h in range(2):
                sm_ref[pl.ds(nod(2, i, j, h), 8), :] = jnp.maximum(
                    s3_ref[pl.ds(nod(2, i, j, h), 8), :], mid
                )

    def flux(src, d, c, i, j, h, off=0):
        if c == 0:
            return src[pl.ds(blk(1 + d, i, j, h) + off, 8), :]
        return f_ref[pl.ds(nod(FLUX_OF[d][c], i, j, h) + off, 8), :]

    def cell(src, c, i, j, h, off=0):
        return src[pl.ds(blk(c, i, j, h) + off, 8), :]

    ex, ey = parity("group"), parity("dev")
    nodal(s_ref)
    for b in range(4):
        for h in range(2):
            for d, g_ref, even_ref, odd_ref, even, bit, step in (
                (0, gx_ref, xe_ref, xo_ref, ex, bx, 2),
                (1, gy_ref, ye_ref, yo_ref, ey, by, 1),
            ):
                first = (0, b) if d == 0 else (b, 0)
                last = (3, b) if d == 0 else (b, 3)
                uf = [cell(s_ref, c, *first, h) for c in range(5)]
                ul = [cell(s_ref, c, *last, h) for c in range(5)]
                he = [even_ref[pl.ds((c * 4 + b) * 8, 8), :] for c in range(5)]
                ho = [odd_ref[pl.ds((c * 4 + b) * 8, 8), :] for c in range(5)]
                hl = [jnp.where(even, ho[c], he[c]) for c in range(5)]
                hh = [jnp.where(even, he[c], ho[c]) for c in range(5)]
                if h == 1:
                    hl = [turn(t, -step) for t in hl]
                    hh = [turn(t, step) for t in hh]
                before = [jnp.where(bit, turn(ul[c], step), hl[c]) for c in range(5)]
                after = [jnp.where(bit, hh[c], turn(uf[c], -step)) for c in range(5)]
                fb, sb = point_flux(before, d)
                fa, sa = point_flux(after, d)
                sl = jnp.maximum(sb, s3_ref[pl.ds(nod(d, *first, h), 8), :])
                sh = jnp.maximum(sa, s3_ref[pl.ds(nod(d, *last, h), 8), :])
                for c in range(5):
                    at = ((c * 4 + b) * 2 + h) * 8
                    g_ref[pl.ds(at, 8), :] = twice_face(
                        fb[c], flux(s_ref, d, c, *first, h), sl, before[c], uf[c]
                    )
                    g_ref[pl.ds(320 + at, 8), :] = twice_face(
                        flux(s_ref, d, c, *last, h), fa[c], sh, ul[c], after[c]
                    )
    for i, j in IJ:
        own = [jnp.where(bk, cell(s_ref, c, i, j, 1), cell(s_ref, c, i, j, 0)) for c in range(5)]
        across = z_wall_pair(own, lane)
        fo, so = point_flux(own, 2)
        fa, sa = point_flux(across, 2)
        s = jnp.maximum(so, sa)
        s = jnp.where(bk, s, -s)
        for c in range(5):
            gz_ref[pl.ds(((c * 4 + i) * 4 + j) * 8, 8), :] = (fo[c] + fa[c]) - s * (across[c] - own[c])

    def gxy(g_ref, side, c, b, h):
        return g_ref[pl.ds(side * 320 + ((c * 4 + b) * 2 + h) * 8, 8), :]

    def gz(c, i, j):
        return gz_ref[pl.ds(((c * 4 + i) * 4 + j) * 8, 8), :]

    table = derivative_table()
    table[0, 0] += 1.0 / WEIGHTS[0]
    table[3, 3] -= 1.0 / WEIGHTS[3]
    table = COURANT * table
    lift = COURANT * 0.5 / WEIGHTS[0]

    def lanes_pair(lo_value, hi_value):
        return jnp.where(bk, float(hi_value), float(lo_value)).astype(F32)

    zc = [
        [lanes_pair(table[2 * h, 2 * g], table[2 * h + 1, 2 * g + 1]) for g in range(2)]
        + [lanes_pair(table[2 * h, 2 * g + 1], table[2 * h + 1, 2 * g]) for g in range(2)]
        for h in range(2)
    ]
    zl = [lanes_pair(-lift, 0.0), lanes_pair(0.0, lift)]

    for c in range(5):
        for h in range(2):
            acc = {}
            for b in range(4):
                for d in range(2):
                    line = [(a, b) if d == 0 else (b, a) for a in range(4)]
                    fl = [flux(s_ref, d, c, *n, h) for n in line]
                    g_ref = gx_ref if d == 0 else gy_ref
                    for a in range(4):
                        r = None
                        for m in range(4):
                            if table[a, m] != 0.0:
                                t = float(table[a, m]) * fl[m]
                                r = t if r is None else r + t
                        if a == 0:
                            r = r - float(lift) * gxy(g_ref, 0, c, b, h)
                        if a == 3:
                            r = r + float(lift) * gxy(g_ref, 1, c, b, h)
                        acc.setdefault(line[a], []).append(r)
            for i, j in IJ:
                fa = flux(s_ref, 2, c, i, j, 0)
                fb = flux(s_ref, 2, c, i, j, 1)
                r = zc[h][0] * fa + zc[h][1] * fb + zc[h][2] * turn(fa, 4) + zc[h][3] * turn(fb, 4)
                r = r + zl[h] * gz(c, i, j)
                r = r + (acc[i, j][0] + acc[i, j][1])
                out_ref[pl.ds(blk(c, i, j, h), 8), :] = cell(s_ref, c, i, j, h) - r

    scale = COURANT / SUBSTEPS * 0.5 / WEIGHTS
    kz = [lanes_pair(scale[0], scale[1]), lanes_pair(scale[2], scale[3])]

    def advance(src, put):
        for c in range(5):
            done = {}
            for h in range(2):
                diff = {}
                for b in range(4):
                    for d in range(2):
                        line = [(a, b) if d == 0 else (b, a) for a in range(4)]
                        g_ref = gx_ref if d == 0 else gy_ref
                        u = [cell(src, c, *n, h) for n in line]
                        f = [flux(src, d, c, *n, h) for n in line]
                        g = [gxy(g_ref, 0, c, b, h)]
                        for a in range(3):
                            g.append(
                                twice_face(
                                    f[a], f[a + 1],
                                    sm_ref[pl.ds(nod(d, *line[a], h), 8), :],
                                    u[a], u[a + 1],
                                )
                            )
                        g.append(gxy(g_ref, 1, c, b, h))
                        for a in range(4):
                            diff[d, line[a]] = g[a + 1] - g[a]
                for i, j in IJ:
                    if scale[i] == scale[j]:
                        r = float(scale[i]) * (diff[0, (i, j)] + diff[1, (i, j)])
                    else:
                        r = float(scale[i]) * diff[0, (i, j)] + float(scale[j]) * diff[1, (i, j)]
                    u = cell(src, c, i, j, h)
                    um = cell(src, c, i, j, 0, 4)
                    fz = flux(src, 2, c, i, j, h)
                    fm = flux(src, 2, c, i, j, 0, 4)
                    s = sm_ref[pl.ds(nod(2, i, j, h), 8), :]
                    if h == 0:
                        t = twice_face(fz, fm, s, u, um)
                        dz = t - jnp.where(low, gz(c, i, j), turn(t, 4))
                    else:
                        t = twice_face(fm, fz, s, um, u)
                        dz = jnp.where(low, turn(t, 4), gz(c, i, j)) - t
                    done[i, j, h] = u - (r + kz[h] * dz)
            for (i, j, h), value in done.items():
                put(c, i, j, h, value)

    def put_u(c, i, j, h, value):
        u_ref[pl.ds(blk(c, i, j, h), 8), :] = value

    def put_out(c, i, j, h, value):
        at = pl.ds(blk(c, i, j, h), 8)
        out_ref[at, :] = jnp.where(troubled, value, out_ref[at, :])

    u_ref[...] = s_ref[...]

    def substep(_, carry):
        advance(u_ref, put_u)
        nodal(u_ref)
        return carry

    lax.fori_loop(0, SUBSTEPS - 1, substep, 0)
    slot = slot_ref[...]
    troubled = jnp.concatenate([slot, slot], axis=0) >= 0
    advance(u_ref, put_out)


def on_device(state, limit_slot, wall_owner, interpret=False):
    n_group, n_dev = lax.axis_size("group"), lax.axis_size("dev")
    devices = n_group * n_dev
    rows = state.reshape(ROWS, 128)
    halo = jax.ShapeDtypeStruct((160, 128), F32)
    vmem = pl.BlockSpec(memory_space=pltpu.VMEM)
    ye, yo, xe, xo, part = pl.pallas_call(
        prepare_kernel,
        out_shape=(halo, halo, halo, halo, jax.ShapeDtypeStruct((devices, SN_DEV), F32)),
        in_specs=[vmem, pl.BlockSpec(memory_space=pltpu.SMEM)],
        out_specs=(vmem,) * 5,
        compiler_params=pltpu.CompilerParams(vmem_limit_bytes=VMEM_LIMIT),
        name="prepare",
        interpret=interpret,
    )(rows, wall_owner)

    def swap(x, axis, odd):
        n = lax.axis_size(axis)
        edges = [(i, (i + 1) % n) for i in range(odd, n, 2)]
        return lax.ppermute(x, axis, edges + [(b, a) for a, b in edges])

    yo = swap(yo, "dev", 1)
    xo = swap(xo, "group", 1)
    ye = swap(ye, "dev", 0)
    xe = swap(xe, "group", 0)
    parts = lax.all_to_all(part, ("group", "dev"), 0, 0, tiled=True)
    wall_loads = jnp.sum(parts, axis=0)
    section = pl.pallas_call(
        section_kernel,
        out_shape=jax.ShapeDtypeStruct((ROWS, 128), F32),
        in_specs=[vmem] * 6,
        out_specs=vmem,
        scratch_shapes=[
            pltpu.VMEM((ROWS, 128), F32),
            pltpu.VMEM((9 * 256, 128), F32),
            pltpu.VMEM((3 * 256, 128), F32),
            pltpu.VMEM((3 * 256, 128), F32),
            pltpu.VMEM((640, 128), F32),
            pltpu.VMEM((640, 128), F32),
            pltpu.VMEM((640, 128), F32),
        ],
        compiler_params=pltpu.CompilerParams(vmem_limit_bytes=VMEM_LIMIT),
        cost_estimate=pl.CostEstimate(flops=60_000_000, transcendentals=600_000, bytes_accessed=2_000_000),
        name="section",
        interpret=interpret,
    )
    out = section(rows, limit_slot.reshape(4, 128), ye, yo, xe, xo)
    return out.reshape(state.shape), wall_loads


def solution(mesh):
    in_specs = (
        P(None, None, None, None, "group", "dev", None),
        P("group", "dev", None),
        P("group", "dev", None),
    )
    out_specs = (P(None, None, None, None, "group", "dev", None), P(("group", "dev")))
    return jax.shard_map(
        on_device, mesh=mesh, in_specs=in_specs, out_specs=out_specs, check_vma=False
    )
```

```python
import jax
import jax.numpy as jnp
import numpy as np
from jax import lax
from jax.experimental import pallas as pl
from jax.experimental.pallas import tpu as pltpu
from jax.sharding import PartitionSpec as P


SUBSTEPS = 8
SN_DEV = 8
GAMMA = 1.4
COURANT = 0.02
F32 = jnp.float32

ROWS = 1280
VMEM_LIMIT = 16 * 1024 * 1024


def blk(v, i, j, h):
    return (((v * 4 + i) * 4 + j) * 2 + h) * 8


def nod(q, i, j, h):
    return q * 256 + ((i * 4 + j) * 2 + h) * 8


FLUX_OF = (
    (None, 0, 1, 2, 6),
    (None, 1, 3, 4, 7),
    (None, 2, 4, 5, 8),
)


def derivative_table():
    gll_nodes = np.array([-1.0, -np.sqrt(0.2), np.sqrt(0.2), 1.0])
    bary = np.array(
        [1.0 / np.prod([gll_nodes[a] - gll_nodes[b] for b in range(4) if b != a]) for a in range(4)]
    )
    table = np.zeros((4, 4))
    for a in range(4):
        for b in range(4):
            if a != b:
                table[a, b] = bary[b] / bary[a] / (gll_nodes[a] - gll_nodes[b])
    for a in (0, 3):
        table[a, a] = -np.sum(table[a])
    return table


WEIGHTS = np.array([1.0, 5.0, 5.0, 1.0]) / 6.0


def row_bit(bit):
    rows = lax.broadcasted_iota(jnp.int32, (8, 128), 0)
    return (rows & bit) != 0


def turn(x, shift):
    return pltpu.roll(x, shift % 8, 0)


def root(x):
    return x * lax.rsqrt(jnp.maximum(x, 1e-30))


def point_flux(u, d):
    inv = 1.0 / u[0]
    v = u[1 + d] * inv
    ke = (u[1] * u[1] + u[2] * u[2] + u[3] * u[3]) * inv
    p = (GAMMA - 1.0) * (u[4] - 0.5 * ke)
    flux = [u[1 + d]] + [u[1 + a] * v for a in range(3)] + [v * (u[4] + p)]
    flux[1 + d] = flux[1 + d] + p
    speed = jnp.abs(v) + root(GAMMA * p * inv)
    return flux, speed


def twice_face(fl, fr, s, ul, ur):
    return (fl + fr) - s * (ur - ul)


def z_wall_pair(own, lane):
    low = jnp.logical_not(row_bit(4))
    wall = (low & (lane == 0)) | (row_bit(4) & (lane == 127))
    across = []
    for c in range(5):
        x = turn(own[c], 4)
        n = jnp.where(low, pltpu.roll(x, 1, 1), pltpu.roll(x, 127, 1))
        across.append(jnp.where(wall, -own[c] if c == 3 else own[c], n))
    return across


def parity(axis):
    return jnp.full((8, 128), lax.axis_index(axis) % 2, jnp.int32) == 0


def prepare_kernel(
    state_ref, owner_ref, ye_ref, yo_ref, xe_ref, xo_ref, part_out_ref, s_ref, own_ref, part_ref, sems
):
    fetch = pltpu.make_async_copy(state_ref, s_ref, sems.at[0])
    fetch_own = pltpu.make_async_copy(owner_ref, own_ref, sems.at[1])
    store_part = pltpu.make_async_copy(part_ref, part_out_ref, sems.at[2])
    fetch.start()
    fetch_own.start()
    part_ref[...] = jnp.zeros(part_ref.shape, F32)
    bx, by, bk = row_bit(2), row_bit(1), row_bit(4)
    lane = lax.broadcasted_iota(jnp.int32, (8, 128), 1)
    ex, ey = parity("group"), parity("dev")
    fetch.wait()
    fetch_own.wait()

    def get(v, i, j, h):
        return s_ref[pl.ds(blk(v, i, j, h), 8), :]

    total = jnp.zeros((8, 128), F32)
    sign = jnp.where(bk, 0.5, -0.5).astype(F32)
    for i in range(4):
        for j in range(4):
            own = [jnp.where(bk, get(c, i, j, 1), get(c, i, j, 0)) for c in range(5)]
            across = list(own)
            across[3] = -own[3]
            fo, so = point_flux(own, 2)
            fa, sa = point_flux(across, 2)
            jump = jnp.where(bk, across[3] - own[3], own[3] - across[3])
            flux = (fo[3] + fa[3]) - jnp.maximum(so, sa) * jump
            total = total + float(WEIGHTS[i] * WEIGHTS[j]) * flux
    at_wall = (bk & (lane == 127)) | (jnp.logical_not(bk) & (lane == 0))
    loads = jnp.sum(jnp.where(at_wall, total * sign, 0.0), axis=1, keepdims=True)
    lane1 = lax.broadcasted_iota(jnp.int32, (1, SN_DEV), 1)
    for side in range(2):
        for x in range(2):
            for y in range(2):
                node = own_ref[x, y, side]
                r = side * 4 + x * 2 + y
                at = pl.ds(node // SN_DEV, 1)
                part_ref[at, :] = part_ref[at, :] + jnp.where(
                    lane1 == node % SN_DEV, loads[r : r + 1, :], 0.0
                )
    store_part.start()
    for c in range(5):
        for a in range(4):
            row = pl.ds((c * 4 + a) * 8, 8)
            top = jnp.where(by, get(c, a, 3, 1), turn(get(c, a, 3, 0), -1))
            low = jnp.where(by, turn(get(c, a, 0, 0), 1), get(c, a, 0, 1))
            ye_ref[row, :] = jnp.where(ey, top, low)
            yo_ref[row, :] = jnp.where(ey, low, top)
            top = jnp.where(bx, get(c, 3, a, 1), turn(get(c, 3, a, 0), -2))
            low = jnp.where(bx, turn(get(c, 0, a, 0), 2), get(c, 0, a, 1))
            xe_ref[row, :] = jnp.where(ex, top, low)
            xo_ref[row, :] = jnp.where(ex, low, top)
    store_part.wait()


def sum_kernel(parts_ref, loads_ref):
    loads_ref[...] = jnp.sum(parts_ref[...], axis=0, keepdims=True)


IJ = [(i, j) for i in range(4) for j in range(4)]


def cell(src, c, i, j, h, off=0):
    return src[pl.ds(blk(c, i, j, h) + off, 8), :]


def flux_of(src, f_ref, d, c, i, j, h, off=0):
    if c == 0:
        return cell(src, 1 + d, i, j, h, off)
    return f_ref[pl.ds(nod(FLUX_OF[d][c], i, j, h) + off, 8), :]


def face_at(g_ref, side, c, b, h):
    return g_ref[pl.ds(side * 320 + ((c * 4 + b) * 2 + h) * 8, 8), :]


def z_face_at(gz_ref, c, i, j):
    return gz_ref[pl.ds(((c * 4 + i) * 4 + j) * 8, 8), :]


def nodal(src, f_ref, s3_ref=None, sm_ref=None):
    for i, j in IJ:
        for h in range(2):
            u = [cell(src, c, i, j, h) for c in range(5)]
            inv = 1.0 / u[0]
            v = [u[1 + d] * inv for d in range(3)]
            xx, xy, xz = u[1] * v[0], u[1] * v[1], u[1] * v[2]
            yy, yz, zz = u[2] * v[1], u[2] * v[2], u[3] * v[2]
            p = (GAMMA - 1.0) * (u[4] - 0.5 * (xx + yy + zz))
            e = u[4] + p
            q = [xx + p, xy, xz, yy + p, yz, zz + p, v[0] * e, v[1] * e, v[2] * e]
            for n in range(9):
                f_ref[pl.ds(nod(n, i, j, h), 8), :] = q[n]
            if s3_ref is not None:
                sound = root(GAMMA * p * inv)
                for d in range(3):
                    s3_ref[pl.ds(nod(d, i, j, h), 8), :] = jnp.abs(v[d]) + sound
    if s3_ref is None:
        return

    def speed(d, i, j, h, off=0):
        return s3_ref[pl.ds(nod(d, i, j, h) + off, 8), :]

    for a in range(3):
        for b in range(4):
            for h in range(2):
                sm_ref[pl.ds(nod(0, a, b, h), 8), :] = jnp.maximum(
                    speed(0, a, b, h), speed(0, a + 1, b, h)
                )
                sm_ref[pl.ds(nod(1, b, a, h), 8), :] = jnp.maximum(
                    speed(1, b, a, h), speed(1, b, a + 1, h)
                )
    for i, j in IJ:
        mid = speed(2, i, j, 0, 4)
        for h in range(2):
            sm_ref[pl.ds(nod(2, i, j, h), 8), :] = jnp.maximum(speed(2, i, j, h), mid)


def pair(lo_value, hi_value):
    return jnp.where(row_bit(4), float(hi_value), float(lo_value)).astype(F32)


LIFT = COURANT * 0.5 / WEIGHTS[0]


def volume_kernel(s_ref, gz_ref, dg_ref, f_ref):
    bk = row_bit(4)
    lane = lax.broadcasted_iota(jnp.int32, (8, 128), 1)
    nodal(s_ref, f_ref)
    for i, j in IJ:
        own = [jnp.where(bk, cell(s_ref, c, i, j, 1), cell(s_ref, c, i, j, 0)) for c in range(5)]
        across = z_wall_pair(own, lane)
        fo, so = point_flux(own, 2)
        fa, sa = point_flux(across, 2)
        s = jnp.maximum(so, sa)
        s = jnp.where(bk, s, -s)
        for c in range(5):
            gz_ref[pl.ds(((c * 4 + i) * 4 + j) * 8, 8), :] = (fo[c] + fa[c]) - s * (across[c] - own[c])

    table = derivative_table()
    table[0, 0] += 1.0 / WEIGHTS[0]
    table[3, 3] -= 1.0 / WEIGHTS[3]
    table = COURANT * table
    zc = [
        [pair(table[2 * h, 2 * g], table[2 * h + 1, 2 * g + 1]) for g in range(2)]
        + [pair(table[2 * h, 2 * g + 1], table[2 * h + 1, 2 * g]) for g in range(2)]
        for h in range(2)
    ]
    zl = [pair(-LIFT, 0.0), pair(0.0, LIFT)]
    for c in range(5):
        for h in range(2):
            acc = {}
            for b in range(4):
                for d in range(2):
                    line = [(a, b) if d == 0 else (b, a) for a in range(4)]
                    fl = [flux_of(s_ref, f_ref, d, c, *n, h) for n in line]
                    for a in range(4):
                        terms = [float(table[a, m]) * fl[m] for m in range(4) if table[a, m] != 0.0]
                        acc.setdefault(line[a], []).append(sum(terms[1:], terms[0]))
            for i, j in IJ:
                fa = flux_of(s_ref, f_ref, 2, c, i, j, 0)
                fb = flux_of(s_ref, f_ref, 2, c, i, j, 1)
                r = zc[h][0] * fa + zc[h][1] * fb + zc[h][2] * turn(fa, 4) + zc[h][3] * turn(fb, 4)
                r = r + zl[h] * z_face_at(gz_ref, c, i, j)
                r = r + (acc[i, j][0] + acc[i, j][1])
                dg_ref[pl.ds(blk(c, i, j, h), 8), :] = cell(s_ref, c, i, j, h) - r


def section_kernel(
    s_ref, slots_ref, ye_ref, yo_ref, xe_ref, xo_ref, gz_ref, dg_ref, result_ref,
    u_ref, f_ref, s3_ref, sm_ref, gx_ref, gy_ref, out_ref, slot_ref, sems,
):
    fetch_slot = pltpu.make_async_copy(slots_ref, slot_ref, sems.at[5])
    fetch_slot.start()
    bx, by, bk = row_bit(2), row_bit(1), row_bit(4)
    low = jnp.logical_not(bk)
    ex, ey = parity("group"), parity("dev")
    nodal(s_ref, f_ref, s3_ref, sm_ref)
    for b in range(4):
        for h in range(2):
            for d, g_ref, even_ref, odd_ref, even, bit, step in (
                (0, gx_ref, xe_ref, xo_ref, ex, bx, 2),
                (1, gy_ref, ye_ref, yo_ref, ey, by, 1),
            ):
                first = (0, b) if d == 0 else (b, 0)
                last = (3, b) if d == 0 else (b, 3)
                uf = [cell(s_ref, c, *first, h) for c in range(5)]
                ul = [cell(s_ref, c, *last, h) for c in range(5)]
                he = [even_ref[pl.ds((c * 4 + b) * 8, 8), :] for c in range(5)]
                ho = [odd_ref[pl.ds((c * 4 + b) * 8, 8), :] for c in range(5)]
                hl = [jnp.where(even, ho[c], he[c]) for c in range(5)]
                hh = [jnp.where(even, he[c], ho[c]) for c in range(5)]
                if h == 1:
                    hl = [turn(t, -step) for t in hl]
                    hh = [turn(t, step) for t in hh]
                before = [jnp.where(bit, turn(ul[c], step), hl[c]) for c in range(5)]
                after = [jnp.where(bit, hh[c], turn(uf[c], -step)) for c in range(5)]
                fb, sb = point_flux(before, d)
                fa, sa = point_flux(after, d)
                sl = jnp.maximum(sb, s3_ref[pl.ds(nod(d, *first, h), 8), :])
                sh = jnp.maximum(sa, s3_ref[pl.ds(nod(d, *last, h), 8), :])
                for c in range(5):
                    at = ((c * 4 + b) * 2 + h) * 8
                    g_ref[pl.ds(at, 8), :] = twice_face(
                        fb[c], flux_of(s_ref, f_ref, d, c, *first, h), sl, before[c], uf[c]
                    )
                    g_ref[pl.ds(320 + at, 8), :] = twice_face(
                        flux_of(s_ref, f_ref, d, c, *last, h), fa[c], sh, ul[c], after[c]
                    )

    scale = COURANT / SUBSTEPS * 0.5 / WEIGHTS
    kz = [pair(scale[0], scale[1]), pair(scale[2], scale[3])]

    def advance(src, put, finish):
        for c in range(5):
            done = {}
            for h in range(2):
                diff = {}
                for b in range(4):
                    for d in range(2):
                        line = [(a, b) if d == 0 else (b, a) for a in range(4)]
                        g_ref = gx_ref if d == 0 else gy_ref
                        u = [cell(src, c, *n, h) for n in line]
                        f = [flux_of(src, f_ref, d, c, *n, h) for n in line]
                        g = [face_at(g_ref, 0, c, b, h)]
                        for a in range(3):
                            s = sm_ref[pl.ds(nod(d, *line[a], h), 8), :]
                            g.append(twice_face(f[a], f[a + 1], s, u[a], u[a + 1]))
                        g.append(face_at(g_ref, 1, c, b, h))
                        for a in range(4):
                            diff[d, line[a]] = g[a + 1] - g[a]
                for i, j in IJ:
                    if scale[i] == scale[j]:
                        r = float(scale[i]) * (diff[0, (i, j)] + diff[1, (i, j)])
                    else:
                        r = float(scale[i]) * diff[0, (i, j)] + float(scale[j]) * diff[1, (i, j)]
                    u = cell(src, c, i, j, h)
                    um = cell(src, c, i, j, 0, 4)
                    fz = flux_of(src, f_ref, 2, c, i, j, h)
                    fm = flux_of(src, f_ref, 2, c, i, j, 0, 4)
                    s = sm_ref[pl.ds(nod(2, i, j, h), 8), :]
                    gz = z_face_at(gz_ref, c, i, j)
                    if h == 0:
                        t = twice_face(fz, fm, s, u, um)
                        dz = t - jnp.where(low, gz, turn(t, 4))
                    else:
                        t = twice_face(fm, fz, s, um, u)
                        dz = jnp.where(low, turn(t, 4), gz) - t
                    done[i, j, h] = u - (r + kz[h] * dz)
            for (i, j, h), value in done.items():
                put(c, i, j, h, value)
            finish(c)

    def put_u(c, i, j, h, value):
        u_ref[pl.ds(blk(c, i, j, h), 8), :] = value

    def put_out(c, i, j, h, value):
        at = pl.ds(blk(c, i, j, h), 8)
        dg = dg_ref[at, :]
        for n, b, g_ref in ((i, j, gx_ref), (j, i, gy_ref)):
            if n == 0:
                dg = dg + float(LIFT) * face_at(g_ref, 0, c, b, h)
            if n == 3:
                dg = dg - float(LIFT) * face_at(g_ref, 1, c, b, h)
        out_ref[at, :] = jnp.where(troubled, value, dg)

    def store(c):
        rows = pl.ds(c * 256, 256)
        return pltpu.make_async_copy(out_ref.at[rows, :], result_ref.at[rows, :], sems.at[c])

    u_ref[...] = s_ref[...]

    def substep(_, carry):
        advance(u_ref, put_u, lambda c: None)
        nodal(u_ref, f_ref, s3_ref, sm_ref)
        return carry

    lax.fori_loop(0, SUBSTEPS - 1, substep, 0)
    fetch_slot.wait()
    slot = slot_ref[...]
    troubled = jnp.concatenate([slot, slot], axis=0) >= 0
    advance(u_ref, put_out, lambda c: store(c).start())
    for c in range(5):
        store(c).wait()


def on_device(state, limit_slot, wall_owner, interpret=False):
    n_group, n_dev = lax.axis_size("group"), lax.axis_size("dev")
    devices = n_group * n_dev
    rows = state.reshape(ROWS, 128)
    halo = jax.ShapeDtypeStruct((160, 128), F32)
    vmem = pl.BlockSpec(memory_space=pltpu.VMEM)
    hbm = pl.BlockSpec(memory_space=pltpu.HBM)
    ye, yo, xe, xo, part = pl.pallas_call(
        prepare_kernel,
        out_shape=(halo, halo, halo, halo, jax.ShapeDtypeStruct((devices, SN_DEV), F32)),
        in_specs=[hbm, hbm],
        out_specs=(vmem,) * 4 + (hbm,),
        scratch_shapes=[
            pltpu.VMEM((ROWS, 128), F32),
            pltpu.SMEM((2, 2, 2), jnp.int32),
            pltpu.VMEM((devices, SN_DEV), F32),
            pltpu.SemaphoreType.DMA((3,)),
        ],
        compiler_params=pltpu.CompilerParams(vmem_limit_bytes=VMEM_LIMIT),
        name="prepare",
        interpret=interpret,
    )(
        pltpu.with_memory_space_constraint(rows, pltpu.HBM),
        pltpu.with_memory_space_constraint(wall_owner, pltpu.HBM),
    )

    def swap(x, axis, odd):
        n = lax.axis_size(axis)
        edges = [(i, (i + 1) % n) for i in range(odd, n, 2)]
        return lax.ppermute(x, axis, edges + [(b, a) for a, b in edges])

    yo = swap(yo, "dev", 1)
    xo = swap(xo, "group", 1)
    ye = swap(ye, "dev", 0)
    xe = swap(xe, "group", 0)
    parts = lax.all_to_all(part, ("group", "dev"), 0, 0, tiled=True)
    wall_loads = pl.pallas_call(
        sum_kernel,
        out_shape=jax.ShapeDtypeStruct((1, SN_DEV), F32),
        in_specs=[vmem],
        out_specs=vmem,
        compiler_params=pltpu.CompilerParams(vmem_limit_bytes=VMEM_LIMIT),
        name="wall_sum",
        interpret=interpret,
    )(parts).reshape(SN_DEV)
    small = pltpu.CompilerParams(vmem_limit_bytes=VMEM_LIMIT)
    volume = pl.pallas_call(
        volume_kernel,
        out_shape=(jax.ShapeDtypeStruct((640, 128), F32), jax.ShapeDtypeStruct((ROWS, 128), F32)),
        in_specs=[vmem],
        out_specs=(vmem, vmem),
        scratch_shapes=[pltpu.VMEM((9 * 256, 128), F32)],
        compiler_params=small,
        name="volume",
        interpret=interpret,
    )
    section = pl.pallas_call(
        section_kernel,
        out_shape=jax.ShapeDtypeStruct((ROWS, 128), F32),
        in_specs=[vmem, hbm] + [vmem] * 6,
        out_specs=hbm,
        scratch_shapes=[
            pltpu.VMEM((ROWS, 128), F32),
            pltpu.VMEM((9 * 256, 128), F32),
            pltpu.VMEM((3 * 256, 128), F32),
            pltpu.VMEM((3 * 256, 128), F32),
            pltpu.VMEM((640, 128), F32),
            pltpu.VMEM((640, 128), F32),
            pltpu.VMEM((ROWS, 128), F32),
            pltpu.VMEM((4, 128), jnp.int32),
            pltpu.SemaphoreType.DMA((6,)),
        ],
        compiler_params=small,
        cost_estimate=pl.CostEstimate(flops=60_000_000, transcendentals=600_000, bytes_accessed=2_000_000),
        name="section",
        interpret=interpret,
    )
    gz, dg = volume(rows)
    slots = pltpu.with_memory_space_constraint(limit_slot.reshape(4, 128), pltpu.HBM)
    out = section(rows, slots, ye, yo, xe, xo, gz, dg)
    return out.reshape(state.shape), wall_loads


def solution(mesh):
    in_specs = (
        P(None, None, None, None, "group", "dev", None),
        P("group", "dev", None),
        P("group", "dev", None),
    )
    out_specs = (P(None, None, None, None, "group", "dev", None), P(("group", "dev")))
    return jax.shard_map(
        on_device, mesh=mesh, in_specs=in_specs, out_specs=out_specs, check_vma=False
    )
```

```python
import jax
import jax.numpy as jnp
import numpy as np
from jax import lax
from jax.experimental import pallas as pl
from jax.experimental.pallas import tpu as pltpu
from jax.sharding import PartitionSpec as P


SUBSTEPS = 8
SN_DEV = 8
GAMMA = 1.4
COURANT = 0.02
F32 = jnp.float32

ROWS = 1280
VMEM_LIMIT = 16 * 1024 * 1024


def blk(v, i, j, h):
    return (((v * 4 + i) * 4 + j) * 2 + h) * 8


def nod(q, i, j, h):
    return q * 256 + ((i * 4 + j) * 2 + h) * 8


FLUX_OF = (
    (None, 0, 1, 2, 6),
    (None, 1, 3, 4, 7),
    (None, 2, 4, 5, 8),
)


def derivative_table():
    gll_nodes = np.array([-1.0, -np.sqrt(0.2), np.sqrt(0.2), 1.0])
    bary = np.array(
        [1.0 / np.prod([gll_nodes[a] - gll_nodes[b] for b in range(4) if b != a]) for a in range(4)]
    )
    table = np.zeros((4, 4))
    for a in range(4):
        for b in range(4):
            if a != b:
                table[a, b] = bary[b] / bary[a] / (gll_nodes[a] - gll_nodes[b])
    for a in (0, 3):
        table[a, a] = -np.sum(table[a])
    return table


WEIGHTS = np.array([1.0, 5.0, 5.0, 1.0]) / 6.0


def row_bit(bit):
    rows = lax.broadcasted_iota(jnp.int32, (8, 128), 0)
    return (rows & bit) != 0


def turn(x, shift):
    return pltpu.roll(x, shift % 8, 0)


def root(x):
    return x * lax.rsqrt(jnp.maximum(x, 1e-30))


def point_flux(u, d):
    inv = 1.0 / u[0]
    v = u[1 + d] * inv
    ke = (u[1] * u[1] + u[2] * u[2] + u[3] * u[3]) * inv
    p = (GAMMA - 1.0) * (u[4] - 0.5 * ke)
    flux = [u[1 + d]] + [u[1 + a] * v for a in range(3)] + [v * (u[4] + p)]
    flux[1 + d] = flux[1 + d] + p
    speed = jnp.abs(v) + root(GAMMA * p * inv)
    return flux, speed


def twice_face(fl, fr, s, ul, ur):
    return (fl + fr) - s * (ur - ul)


def z_wall_pair(own, lane):
    low = jnp.logical_not(row_bit(4))
    wall = (low & (lane == 0)) | (row_bit(4) & (lane == 127))
    across = []
    for c in range(5):
        x = turn(own[c], 4)
        n = jnp.where(low, pltpu.roll(x, 1, 1), pltpu.roll(x, 127, 1))
        across.append(jnp.where(wall, -own[c] if c == 3 else own[c], n))
    return across


def parity(axis):
    return jnp.full((8, 128), lax.axis_index(axis) % 2, jnp.int32) == 0


def prepare_kernel(
    state_ref, owner_ref, ye_ref, yo_ref, xe_ref, xo_ref, part_out_ref, s_ref, own_ref, part_ref, sems
):
    fetch = pltpu.make_async_copy(state_ref, s_ref, sems.at[0])
    fetch_own = pltpu.make_async_copy(owner_ref, own_ref, sems.at[1])
    store_part = pltpu.make_async_copy(part_ref, part_out_ref, sems.at[2])
    fetch.start()
    fetch_own.start()
    part_ref[...] = jnp.zeros(part_ref.shape, F32)
    bx, by, bk = row_bit(2), row_bit(1), row_bit(4)
    lane = lax.broadcasted_iota(jnp.int32, (8, 128), 1)
    ex, ey = parity("group"), parity("dev")
    fetch.wait()
    fetch_own.wait()

    def get(v, i, j, h):
        return s_ref[pl.ds(blk(v, i, j, h), 8), :]

    total = jnp.zeros((8, 128), F32)
    sign = jnp.where(bk, 0.5, -0.5).astype(F32)
    for i in range(4):
        for j in range(4):
            own = [jnp.where(bk, get(c, i, j, 1), get(c, i, j, 0)) for c in range(5)]
            fo, so = point_flux(own, 2)
            flux = 2.0 * (fo[3] + jnp.where(bk, so, -so) * own[3])
            total = total + float(WEIGHTS[i] * WEIGHTS[j]) * flux
    at_wall = (bk & (lane == 127)) | (jnp.logical_not(bk) & (lane == 0))
    loads = jnp.sum(jnp.where(at_wall, total * sign, 0.0), axis=1, keepdims=True)
    lane1 = lax.broadcasted_iota(jnp.int32, (1, SN_DEV), 1)
    for side in range(2):
        for x in range(2):
            for y in range(2):
                node = own_ref[x, y, side]
                r = side * 4 + x * 2 + y
                at = pl.ds(node // SN_DEV, 1)
                part_ref[at, :] = part_ref[at, :] + jnp.where(
                    lane1 == node % SN_DEV, loads[r : r + 1, :], 0.0
                )
    store_part.start()
    for c in range(5):
        for a in range(4):
            row = pl.ds((c * 4 + a) * 8, 8)
            top = jnp.where(by, get(c, a, 3, 1), turn(get(c, a, 3, 0), -1))
            low = jnp.where(by, turn(get(c, a, 0, 0), 1), get(c, a, 0, 1))
            ye_ref[row, :] = jnp.where(ey, top, low)
            yo_ref[row, :] = jnp.where(ey, low, top)
            top = jnp.where(bx, get(c, 3, a, 1), turn(get(c, 3, a, 0), -2))
            low = jnp.where(bx, turn(get(c, 0, a, 0), 2), get(c, 0, a, 1))
            xe_ref[row, :] = jnp.where(ex, top, low)
            xo_ref[row, :] = jnp.where(ex, low, top)
    store_part.wait()


def sum_kernel(parts_ref, loads_ref):
    loads_ref[...] = jnp.sum(parts_ref[...], axis=0, keepdims=True)


IJ = [(i, j) for i in range(4) for j in range(4)]


def cell(src, c, i, j, h, off=0):
    return src[pl.ds(blk(c, i, j, h) + off, 8), :]


def flux_of(src, f_ref, d, c, i, j, h, off=0):
    if c == 0:
        return cell(src, 1 + d, i, j, h, off)
    return f_ref[pl.ds(nod(FLUX_OF[d][c], i, j, h) + off, 8), :]


def face_at(g_ref, side, c, b, h):
    return g_ref[pl.ds(side * 320 + ((c * 4 + b) * 2 + h) * 8, 8), :]


def z_face_at(gz_ref, c, i, j):
    return gz_ref[pl.ds(((c * 4 + i) * 4 + j) * 8, 8), :]


def nodal(src, f_ref, s3_ref=None, sm_ref=None):
    for i, j in IJ:
        for h in range(2):
            u = [cell(src, c, i, j, h) for c in range(5)]
            inv = 1.0 / u[0]
            v = [u[1 + d] * inv for d in range(3)]
            xx, xy, xz = u[1] * v[0], u[1] * v[1], u[1] * v[2]
            yy, yz, zz = u[2] * v[1], u[2] * v[2], u[3] * v[2]
            p = (GAMMA - 1.0) * (u[4] - 0.5 * (xx + yy + zz))
            e = u[4] + p
            q = [xx + p, xy, xz, yy + p, yz, zz + p, v[0] * e, v[1] * e, v[2] * e]
            for n in range(9):
                f_ref[pl.ds(nod(n, i, j, h), 8), :] = q[n]
            if s3_ref is not None:
                sound = root(GAMMA * p * inv)
                for d in range(3):
                    s3_ref[pl.ds(nod(d, i, j, h), 8), :] = jnp.abs(v[d]) + sound
    if s3_ref is None:
        return

    def speed(d, i, j, h, off=0):
        return s3_ref[pl.ds(nod(d, i, j, h) + off, 8), :]

    for a in range(3):
        for b in range(4):
            for h in range(2):
                sm_ref[pl.ds(nod(0, a, b, h), 8), :] = jnp.maximum(
                    speed(0, a, b, h), speed(0, a + 1, b, h)
                )
                sm_ref[pl.ds(nod(1, b, a, h), 8), :] = jnp.maximum(
                    speed(1, b, a, h), speed(1, b, a + 1, h)
                )
    for i, j in IJ:
        mid = speed(2, i, j, 0, 4)
        for h in range(2):
            sm_ref[pl.ds(nod(2, i, j, h), 8), :] = jnp.maximum(speed(2, i, j, h), mid)


def pair(lo_value, hi_value):
    return jnp.where(row_bit(4), float(hi_value), float(lo_value)).astype(F32)


LIFT = COURANT * 0.5 / WEIGHTS[0]


SCALE = COURANT / SUBSTEPS * 0.5 / WEIGHTS


def advance(src, f_ref, sm_ref, gx_ref, gy_ref, gz_ref, put, finish=None):
    low = jnp.logical_not(row_bit(4))
    kz = [pair(SCALE[0], SCALE[1]), pair(SCALE[2], SCALE[3])]
    for c in range(5):
        done = {}
        for h in range(2):
            diff = {}
            for b in range(4):
                for d in range(2):
                    line = [(a, b) if d == 0 else (b, a) for a in range(4)]
                    g_ref = gx_ref if d == 0 else gy_ref
                    u = [cell(src, c, *n, h) for n in line]
                    f = [flux_of(src, f_ref, d, c, *n, h) for n in line]
                    g = []
                    for a in range(3):
                        s = sm_ref[pl.ds(nod(d, *line[a], h), 8), :]
                        g.append(twice_face(f[a], f[a + 1], s, u[a], u[a + 1]))
                    if g_ref is None:
                        diff[d, line[0]], diff[d, line[3]] = g[0], -g[2]
                    else:
                        diff[d, line[0]] = g[0] - face_at(g_ref, 0, c, b, h)
                        diff[d, line[3]] = face_at(g_ref, 1, c, b, h) - g[2]
                    diff[d, line[1]], diff[d, line[2]] = g[1] - g[0], g[2] - g[1]
            for i, j in IJ:
                if SCALE[i] == SCALE[j]:
                    r = float(SCALE[i]) * (diff[0, (i, j)] + diff[1, (i, j)])
                else:
                    r = float(SCALE[i]) * diff[0, (i, j)] + float(SCALE[j]) * diff[1, (i, j)]
                u = cell(src, c, i, j, h)
                um = cell(src, c, i, j, 0, 4)
                fz = flux_of(src, f_ref, 2, c, i, j, h)
                fm = flux_of(src, f_ref, 2, c, i, j, 0, 4)
                s = sm_ref[pl.ds(nod(2, i, j, h), 8), :]
                gz = z_face_at(gz_ref, c, i, j)
                if h == 0:
                    t = twice_face(fz, fm, s, u, um)
                    dz = t - jnp.where(low, gz, turn(t, 4))
                else:
                    t = twice_face(fm, fz, s, um, u)
                    dz = jnp.where(low, turn(t, 4), gz) - t
                done[i, j, h] = u - (r + kz[h] * dz)
        for (i, j, h), value in done.items():
            put(c, i, j, h, value)
        if finish is not None:
            finish(c)


def outer_faces(value, factor, gx_ref, gy_ref, c, i, j, h):
    for n, b, g_ref in ((i, j, gx_ref), (j, i, gy_ref)):
        if n == 0:
            value = value + float(factor) * face_at(g_ref, 0, c, b, h)
        if n == 3:
            value = value - float(factor) * face_at(g_ref, 1, c, b, h)
    return value


def volume_kernel(s_ref, gz_ref, dg_ref, u_ref, f_ref, s3_ref, sm_ref):
    bk = row_bit(4)
    lane = lax.broadcasted_iota(jnp.int32, (8, 128), 1)
    nodal(s_ref, f_ref, s3_ref, sm_ref)
    for i, j in IJ:
        own = [jnp.where(bk, cell(s_ref, c, i, j, 1), cell(s_ref, c, i, j, 0)) for c in range(5)]
        across = z_wall_pair(own, lane)
        fo, so = point_flux(own, 2)
        fa, sa = point_flux(across, 2)
        s = jnp.maximum(so, sa)
        s = jnp.where(bk, s, -s)
        for c in range(5):
            gz_ref[pl.ds(((c * 4 + i) * 4 + j) * 8, 8), :] = (fo[c] + fa[c]) - s * (across[c] - own[c])

    table = derivative_table()
    table[0, 0] += 1.0 / WEIGHTS[0]
    table[3, 3] -= 1.0 / WEIGHTS[3]
    table = COURANT * table
    zc = [
        [pair(table[2 * h, 2 * g], table[2 * h + 1, 2 * g + 1]) for g in range(2)]
        + [pair(table[2 * h, 2 * g + 1], table[2 * h + 1, 2 * g]) for g in range(2)]
        for h in range(2)
    ]
    zl = [pair(-LIFT, 0.0), pair(0.0, LIFT)]
    for c in range(5):
        for h in range(2):
            acc = {}
            for b in range(4):
                for d in range(2):
                    line = [(a, b) if d == 0 else (b, a) for a in range(4)]
                    fl = [flux_of(s_ref, f_ref, d, c, *n, h) for n in line]
                    for a in range(4):
                        terms = [float(table[a, m]) * fl[m] for m in range(4) if table[a, m] != 0.0]
                        acc.setdefault(line[a], []).append(sum(terms[1:], terms[0]))
            for i, j in IJ:
                fa = flux_of(s_ref, f_ref, 2, c, i, j, 0)
                fb = flux_of(s_ref, f_ref, 2, c, i, j, 1)
                r = zc[h][0] * fa + zc[h][1] * fb + zc[h][2] * turn(fa, 4) + zc[h][3] * turn(fb, 4)
                r = r + zl[h] * z_face_at(gz_ref, c, i, j)
                r = r + (acc[i, j][0] + acc[i, j][1])
                dg_ref[pl.ds(blk(c, i, j, h), 8), :] = cell(s_ref, c, i, j, h) - r

    def put(c, i, j, h, value):
        u_ref[pl.ds(blk(c, i, j, h), 8), :] = value

    advance(s_ref, f_ref, sm_ref, None, None, gz_ref, put)


def section_kernel(
    s_ref, slots_ref, ye_ref, yo_ref, xe_ref, xo_ref, gz_ref, dg_ref, first_ref, result_ref,
    u_ref, f_ref, s3_ref, sm_ref, gx_ref, gy_ref, out_ref, slot_ref, sems,
):
    fetch_slot = pltpu.make_async_copy(slots_ref, slot_ref, sems.at[5])
    fetch_slot.start()
    bx, by = row_bit(2), row_bit(1)
    ex, ey = parity("group"), parity("dev")
    for b in range(4):
        for h in range(2):
            for d, g_ref, even_ref, odd_ref, even, bit, step in (
                (0, gx_ref, xe_ref, xo_ref, ex, bx, 2),
                (1, gy_ref, ye_ref, yo_ref, ey, by, 1),
            ):
                first = (0, b) if d == 0 else (b, 0)
                last = (3, b) if d == 0 else (b, 3)
                uf = [cell(s_ref, c, *first, h) for c in range(5)]
                ul = [cell(s_ref, c, *last, h) for c in range(5)]
                he = [even_ref[pl.ds((c * 4 + b) * 8, 8), :] for c in range(5)]
                ho = [odd_ref[pl.ds((c * 4 + b) * 8, 8), :] for c in range(5)]
                hl = [jnp.where(even, ho[c], he[c]) for c in range(5)]
                hh = [jnp.where(even, he[c], ho[c]) for c in range(5)]
                if h == 1:
                    hl = [turn(t, -step) for t in hl]
                    hh = [turn(t, step) for t in hh]
                before = [jnp.where(bit, turn(ul[c], step), hl[c]) for c in range(5)]
                after = [jnp.where(bit, hh[c], turn(uf[c], -step)) for c in range(5)]
                fb, sb = point_flux(before, d)
                fa, sa = point_flux(after, d)
                ff, sf = point_flux(uf, d)
                fl, sl = point_flux(ul, d)
                for c in range(5):
                    at = ((c * 4 + b) * 2 + h) * 8
                    g_ref[pl.ds(at, 8), :] = twice_face(
                        fb[c], ff[c], jnp.maximum(sb, sf), before[c], uf[c]
                    )
                    g_ref[pl.ds(320 + at, 8), :] = twice_face(
                        fl[c], fa[c], jnp.maximum(sa, sl), ul[c], after[c]
                    )

    def put_u(c, i, j, h, value):
        u_ref[pl.ds(blk(c, i, j, h), 8), :] = value

    def put_out(c, i, j, h, value):
        at = pl.ds(blk(c, i, j, h), 8)
        dg = outer_faces(dg_ref[at, :], LIFT, gx_ref, gy_ref, c, i, j, h)
        out_ref[at, :] = jnp.where(troubled, value, dg)

    def store(c):
        rows = pl.ds(c * 256, 256)
        return pltpu.make_async_copy(out_ref.at[rows, :], result_ref.at[rows, :], sems.at[c])

    for c in range(5):
        for i, j in IJ:
            for h in range(2):
                value = first_ref[pl.ds(blk(c, i, j, h), 8), :]
                put_u(c, i, j, h, outer_faces(value, SCALE[0], gx_ref, gy_ref, c, i, j, h))
    nodal(u_ref, f_ref, s3_ref, sm_ref)

    def substep(_, carry):
        advance(u_ref, f_ref, sm_ref, gx_ref, gy_ref, gz_ref, put_u)
        nodal(u_ref, f_ref, s3_ref, sm_ref)
        return carry

    lax.fori_loop(0, SUBSTEPS - 2, substep, 0)
    fetch_slot.wait()
    slot = slot_ref[...]
    troubled = jnp.concatenate([slot, slot], axis=0) >= 0
    advance(
        u_ref, f_ref, sm_ref, gx_ref, gy_ref, gz_ref, put_out, lambda c: store(c).start()
    )
    for c in range(5):
        store(c).wait()


def on_device(state, limit_slot, wall_owner, interpret=False):
    n_group, n_dev = lax.axis_size("group"), lax.axis_size("dev")
    devices = n_group * n_dev
    rows = state.reshape(ROWS, 128)
    halo = jax.ShapeDtypeStruct((160, 128), F32)
    vmem = pl.BlockSpec(memory_space=pltpu.VMEM)
    hbm = pl.BlockSpec(memory_space=pltpu.HBM)
    ye, yo, xe, xo, part = pl.pallas_call(
        prepare_kernel,
        out_shape=(halo, halo, halo, halo, jax.ShapeDtypeStruct((devices, SN_DEV), F32)),
        in_specs=[hbm, hbm],
        out_specs=(vmem,) * 4 + (hbm,),
        scratch_shapes=[
            pltpu.VMEM((ROWS, 128), F32),
            pltpu.SMEM((2, 2, 2), jnp.int32),
            pltpu.VMEM((devices, SN_DEV), F32),
            pltpu.SemaphoreType.DMA((3,)),
        ],
        compiler_params=pltpu.CompilerParams(vmem_limit_bytes=VMEM_LIMIT),
        name="prepare",
        interpret=interpret,
    )(
        pltpu.with_memory_space_constraint(rows, pltpu.HBM),
        pltpu.with_memory_space_constraint(wall_owner, pltpu.HBM),
    )

    def swap(x, axis, odd):
        n = lax.axis_size(axis)
        edges = [(i, (i + 1) % n) for i in range(odd, n, 2)]
        return lax.ppermute(x, axis, edges + [(b, a) for a, b in edges])

    yo = swap(yo, "dev", 1)
    xo = swap(xo, "group", 1)
    ye = swap(ye, "dev", 0)
    xe = swap(xe, "group", 0)
    parts = lax.all_to_all(part, ("group", "dev"), 0, 0, tiled=True)
    wall_loads = pl.pallas_call(
        sum_kernel,
        out_shape=jax.ShapeDtypeStruct((1, SN_DEV), F32),
        in_specs=[vmem],
        out_specs=vmem,
        compiler_params=pltpu.CompilerParams(vmem_limit_bytes=VMEM_LIMIT),
        name="wall_sum",
        interpret=interpret,
    )(parts).reshape(SN_DEV)
    small = pltpu.CompilerParams(vmem_limit_bytes=VMEM_LIMIT)
    volume = pl.pallas_call(
        volume_kernel,
        out_shape=(
            jax.ShapeDtypeStruct((640, 128), F32),
            jax.ShapeDtypeStruct((ROWS, 128), F32),
            jax.ShapeDtypeStruct((ROWS, 128), F32),
        ),
        in_specs=[vmem],
        out_specs=(vmem,) * 3,
        scratch_shapes=[
            pltpu.VMEM((9 * 256, 128), F32),
            pltpu.VMEM((3 * 256, 128), F32),
            pltpu.VMEM((3 * 256, 128), F32),
        ],
        compiler_params=small,
        name="volume",
        interpret=interpret,
    )
    section = pl.pallas_call(
        section_kernel,
        out_shape=jax.ShapeDtypeStruct((ROWS, 128), F32),
        in_specs=[vmem, hbm] + [vmem] * 7,
        out_specs=hbm,
        scratch_shapes=[
            pltpu.VMEM((ROWS, 128), F32),
            pltpu.VMEM((9 * 256, 128), F32),
            pltpu.VMEM((3 * 256, 128), F32),
            pltpu.VMEM((3 * 256, 128), F32),
            pltpu.VMEM((640, 128), F32),
            pltpu.VMEM((640, 128), F32),
            pltpu.VMEM((ROWS, 128), F32),
            pltpu.VMEM((4, 128), jnp.int32),
            pltpu.SemaphoreType.DMA((6,)),
        ],
        compiler_params=small,
        cost_estimate=pl.CostEstimate(flops=60_000_000, transcendentals=600_000, bytes_accessed=2_000_000),
        name="section",
        interpret=interpret,
    )
    gz, dg, first = volume(rows)
    slots = pltpu.with_memory_space_constraint(limit_slot.reshape(4, 128), pltpu.HBM)
    out = section(rows, slots, ye, yo, xe, xo, gz, dg, first)
    return out.reshape(state.shape), wall_loads


def solution(mesh):
    in_specs = (
        P(None, None, None, None, "group", "dev", None),
        P("group", "dev", None),
        P("group", "dev", None),
    )
    out_specs = (P(None, None, None, None, "group", "dev", None), P(("group", "dev")))
    return jax.shard_map(
        on_device, mesh=mesh, in_specs=in_specs, out_specs=out_specs, check_vma=False
    )
```

```python
import jax
import jax.numpy as jnp
import numpy as np
from jax import lax
from jax.experimental import pallas as pl
from jax.experimental.pallas import tpu as pltpu
from jax.sharding import PartitionSpec as P


SUBSTEPS = 8
SN_DEV = 8
GAMMA = 1.4
COURANT = 0.02
F32 = jnp.float32

ROWS = 1280
VMEM_LIMIT = 16 * 1024 * 1024


def blk(v, i, j, h):
    return (((v * 4 + i) * 4 + j) * 2 + h) * 8


def nod(q, i, j, h):
    return q * 256 + ((i * 4 + j) * 2 + h) * 8


FLUX_OF = (
    (None, 0, 1, 2, 6),
    (None, 1, 3, 4, 7),
    (None, 2, 4, 5, 8),
)


def derivative_table():
    gll_nodes = np.array([-1.0, -np.sqrt(0.2), np.sqrt(0.2), 1.0])
    bary = np.array(
        [1.0 / np.prod([gll_nodes[a] - gll_nodes[b] for b in range(4) if b != a]) for a in range(4)]
    )
    table = np.zeros((4, 4))
    for a in range(4):
        for b in range(4):
            if a != b:
                table[a, b] = bary[b] / bary[a] / (gll_nodes[a] - gll_nodes[b])
    for a in (0, 3):
        table[a, a] = -np.sum(table[a])
    return table


WEIGHTS = np.array([1.0, 5.0, 5.0, 1.0]) / 6.0


def row_bit(bit):
    rows = lax.broadcasted_iota(jnp.int32, (8, 128), 0)
    return (rows & bit) != 0


def turn(x, shift):
    return pltpu.roll(x, shift % 8, 0)


def root(x):
    return x * lax.rsqrt(jnp.maximum(x, 1e-30))


def point_flux(u, d):
    inv = 1.0 / u[0]
    v = u[1 + d] * inv
    ke = (u[1] * u[1] + u[2] * u[2] + u[3] * u[3]) * inv
    p = (GAMMA - 1.0) * (u[4] - 0.5 * ke)
    flux = [u[1 + d]] + [u[1 + a] * v for a in range(3)] + [v * (u[4] + p)]
    flux[1 + d] = flux[1 + d] + p
    speed = jnp.abs(v) + root(GAMMA * p * inv)
    return flux, speed


def twice_face(fl, fr, s, ul, ur):
    return (fl + fr) - s * (ur - ul)


def z_wall_pair(own, lane):
    low = jnp.logical_not(row_bit(4))
    wall = (low & (lane == 0)) | (row_bit(4) & (lane == 127))
    across = []
    for c in range(5):
        x = turn(own[c], 4)
        n = jnp.where(low, pltpu.roll(x, 1, 1), pltpu.roll(x, 127, 1))
        across.append(jnp.where(wall, -own[c] if c == 3 else own[c], n))
    return across


def parity(axis):
    return jnp.full((8, 128), lax.axis_index(axis) % 2, jnp.int32) == 0


def prepare_kernel(
    state_ref, owner_ref, ye_ref, yo_ref, xe_ref, xo_ref, part_out_ref, s_ref, own_ref, part_ref, sems
):
    def fetch(c):
        rows = pl.ds(c * 256, 256)
        return pltpu.make_async_copy(state_ref.at[rows, :], s_ref.at[rows, :], sems.at[c])

    fetch_own = pltpu.make_async_copy(owner_ref, own_ref, sems.at[5])
    store_part = pltpu.make_async_copy(part_ref, part_out_ref, sems.at[6])
    for c in range(5):
        fetch(c).start()
    fetch_own.start()
    part_ref[...] = jnp.zeros(part_ref.shape, F32)
    bx, by, bk = row_bit(2), row_bit(1), row_bit(4)
    lane = lax.broadcasted_iota(jnp.int32, (8, 128), 1)
    ex, ey = parity("group"), parity("dev")
    for c in range(5):
        fetch(c).wait()
    fetch_own.wait()

    def get(v, i, j, h):
        return s_ref[pl.ds(blk(v, i, j, h), 8), :]

    total = jnp.zeros((8, 128), F32)
    sign = jnp.where(bk, 0.5, -0.5).astype(F32)
    for i in range(4):
        for j in range(4):
            own = [jnp.where(bk, get(c, i, j, 1), get(c, i, j, 0)) for c in range(5)]
            fo, so = point_flux(own, 2)
            flux = 2.0 * (fo[3] + jnp.where(bk, so, -so) * own[3])
            total = total + float(WEIGHTS[i] * WEIGHTS[j]) * flux
    at_wall = (bk & (lane == 127)) | (jnp.logical_not(bk) & (lane == 0))
    loads = jnp.sum(jnp.where(at_wall, total * sign, 0.0), axis=1, keepdims=True)
    lane1 = lax.broadcasted_iota(jnp.int32, (1, SN_DEV), 1)
    for side in range(2):
        for x in range(2):
            for y in range(2):
                node = own_ref[x, y, side]
                r = side * 4 + x * 2 + y
                at = pl.ds(node // SN_DEV, 1)
                part_ref[at, :] = part_ref[at, :] + jnp.where(
                    lane1 == node % SN_DEV, loads[r : r + 1, :], 0.0
                )
    store_part.start()
    for c in range(5):
        for a in range(4):
            row = pl.ds((c * 4 + a) * 8, 8)
            top = jnp.where(by, get(c, a, 3, 1), turn(get(c, a, 3, 0), -1))
            low = jnp.where(by, turn(get(c, a, 0, 0), 1), get(c, a, 0, 1))
            ye_ref[row, :] = jnp.where(ey, top, low)
            yo_ref[row, :] = jnp.where(ey, low, top)
            top = jnp.where(bx, get(c, 3, a, 1), turn(get(c, 3, a, 0), -2))
            low = jnp.where(bx, turn(get(c, 0, a, 0), 2), get(c, 0, a, 1))
            xe_ref[row, :] = jnp.where(ex, top, low)
            xo_ref[row, :] = jnp.where(ex, low, top)
    store_part.wait()


def sum_kernel(parts_ref, loads_ref):
    loads_ref[...] = jnp.sum(parts_ref[...], axis=0, keepdims=True)


IJ = [(i, j) for i in range(4) for j in range(4)]


def cell(src, c, i, j, h, off=0):
    return src[pl.ds(blk(c, i, j, h) + off, 8), :]


def flux_of(src, f_ref, d, c, i, j, h, off=0):
    if c == 0:
        return cell(src, 1 + d, i, j, h, off)
    return f_ref[pl.ds(nod(FLUX_OF[d][c], i, j, h) + off, 8), :]


def face_at(g_ref, side, c, b, h):
    return g_ref[pl.ds(side * 320 + ((c * 4 + b) * 2 + h) * 8, 8), :]


def z_face_at(gz_ref, c, i, j):
    return gz_ref[pl.ds(((c * 4 + i) * 4 + j) * 8, 8), :]


def nodal(src, f_ref, s3_ref=None, sm_ref=None):
    for i, j in IJ:
        for h in range(2):
            u = [cell(src, c, i, j, h) for c in range(5)]
            inv = 1.0 / u[0]
            v = [u[1 + d] * inv for d in range(3)]
            xx, xy, xz = u[1] * v[0], u[1] * v[1], u[1] * v[2]
            yy, yz, zz = u[2] * v[1], u[2] * v[2], u[3] * v[2]
            p = (GAMMA - 1.0) * (u[4] - 0.5 * (xx + yy + zz))
            e = u[4] + p
            q = [xx + p, xy, xz, yy + p, yz, zz + p, v[0] * e, v[1] * e, v[2] * e]
            for n in range(9):
                f_ref[pl.ds(nod(n, i, j, h), 8), :] = q[n]
            if s3_ref is not None:
                sound = root(GAMMA * p * inv)
                for d in range(3):
                    s3_ref[pl.ds(nod(d, i, j, h), 8), :] = jnp.abs(v[d]) + sound
    if s3_ref is None:
        return

    def speed(d, i, j, h, off=0):
        return s3_ref[pl.ds(nod(d, i, j, h) + off, 8), :]

    for a in range(3):
        for b in range(4):
            for h in range(2):
                sm_ref[pl.ds(nod(0, a, b, h), 8), :] = jnp.maximum(
                    speed(0, a, b, h), speed(0, a + 1, b, h)
                )
                sm_ref[pl.ds(nod(1, b, a, h), 8), :] = jnp.maximum(
                    speed(1, b, a, h), speed(1, b, a + 1, h)
                )
    for i, j in IJ:
        mid = speed(2, i, j, 0, 4)
        for h in range(2):
            sm_ref[pl.ds(nod(2, i, j, h), 8), :] = jnp.maximum(speed(2, i, j, h), mid)


def pair(lo_value, hi_value):
    return jnp.where(row_bit(4), float(hi_value), float(lo_value)).astype(F32)


LIFT = COURANT * 0.5 / WEIGHTS[0]


SCALE = COURANT / SUBSTEPS * 0.5 / WEIGHTS


def advance(src, f_ref, sm_ref, gx_ref, gy_ref, gz_ref, put, finish=None):
    low = jnp.logical_not(row_bit(4))
    kz = [pair(SCALE[0], SCALE[1]), pair(SCALE[2], SCALE[3])]
    for c in range(5):
        done = {}
        for h in range(2):
            diff = {}
            for b in range(4):
                for d in range(2):
                    line = [(a, b) if d == 0 else (b, a) for a in range(4)]
                    g_ref = gx_ref if d == 0 else gy_ref
                    u = [cell(src, c, *n, h) for n in line]
                    f = [flux_of(src, f_ref, d, c, *n, h) for n in line]
                    g = []
                    for a in range(3):
                        s = sm_ref[pl.ds(nod(d, *line[a], h), 8), :]
                        g.append(twice_face(f[a], f[a + 1], s, u[a], u[a + 1]))
                    if g_ref is None:
                        diff[d, line[0]], diff[d, line[3]] = g[0], -g[2]
                    else:
                        diff[d, line[0]] = g[0] - face_at(g_ref, 0, c, b, h)
                        diff[d, line[3]] = face_at(g_ref, 1, c, b, h) - g[2]
                    diff[d, line[1]], diff[d, line[2]] = g[1] - g[0], g[2] - g[1]
            for i, j in IJ:
                if SCALE[i] == SCALE[j]:
                    r = float(SCALE[i]) * (diff[0, (i, j)] + diff[1, (i, j)])
                else:
                    r = float(SCALE[i]) * diff[0, (i, j)] + float(SCALE[j]) * diff[1, (i, j)]
                u = cell(src, c, i, j, h)
                um = cell(src, c, i, j, 0, 4)
                fz = flux_of(src, f_ref, 2, c, i, j, h)
                fm = flux_of(src, f_ref, 2, c, i, j, 0, 4)
                s = sm_ref[pl.ds(nod(2, i, j, h), 8), :]
                gz = z_face_at(gz_ref, c, i, j)
                if h == 0:
                    t = twice_face(fz, fm, s, u, um)
                    dz = t - jnp.where(low, gz, turn(t, 4))
                else:
                    t = twice_face(fm, fz, s, um, u)
                    dz = jnp.where(low, turn(t, 4), gz) - t
                done[i, j, h] = u - (r + kz[h] * dz)
        for (i, j, h), value in done.items():
            put(c, i, j, h, value)
        if finish is not None:
            finish(c)


def outer_faces(value, factor, gx_ref, gy_ref, c, i, j, h):
    for n, b, g_ref in ((i, j, gx_ref), (j, i, gy_ref)):
        if n == 0:
            value = value + float(factor) * face_at(g_ref, 0, c, b, h)
        if n == 3:
            value = value - float(factor) * face_at(g_ref, 1, c, b, h)
    return value


def volume_kernel(s_ref, gz_ref, dg_ref, u_ref, f_ref, s3_ref, sm_ref):
    bk = row_bit(4)
    lane = lax.broadcasted_iota(jnp.int32, (8, 128), 1)
    nodal(s_ref, f_ref, s3_ref, sm_ref)
    for i, j in IJ:
        own = [jnp.where(bk, cell(s_ref, c, i, j, 1), cell(s_ref, c, i, j, 0)) for c in range(5)]
        across = z_wall_pair(own, lane)
        fo, so = point_flux(own, 2)
        fa, sa = point_flux(across, 2)
        s = jnp.maximum(so, sa)
        s = jnp.where(bk, s, -s)
        for c in range(5):
            gz_ref[pl.ds(((c * 4 + i) * 4 + j) * 8, 8), :] = (fo[c] + fa[c]) - s * (across[c] - own[c])

    table = derivative_table()
    table[0, 0] += 1.0 / WEIGHTS[0]
    table[3, 3] -= 1.0 / WEIGHTS[3]
    table = COURANT * table
    zc = [
        [pair(table[2 * h, 2 * g], table[2 * h + 1, 2 * g + 1]) for g in range(2)]
        + [pair(table[2 * h, 2 * g + 1], table[2 * h + 1, 2 * g]) for g in range(2)]
        for h in range(2)
    ]
    zl = [pair(-LIFT, 0.0), pair(0.0, LIFT)]
    for c in range(5):
        for h in range(2):
            acc = {}
            for b in range(4):
                for d in range(2):
                    line = [(a, b) if d == 0 else (b, a) for a in range(4)]
                    fl = [flux_of(s_ref, f_ref, d, c, *n, h) for n in line]
                    for a in range(4):
                        terms = [float(table[a, m]) * fl[m] for m in range(4) if table[a, m] != 0.0]
                        acc.setdefault(line[a], []).append(sum(terms[1:], terms[0]))
            for i, j in IJ:
                fa = flux_of(s_ref, f_ref, 2, c, i, j, 0)
                fb = flux_of(s_ref, f_ref, 2, c, i, j, 1)
                r = zc[h][0] * fa + zc[h][1] * fb + zc[h][2] * turn(fa, 4) + zc[h][3] * turn(fb, 4)
                r = r + zl[h] * z_face_at(gz_ref, c, i, j)
                r = r + (acc[i, j][0] + acc[i, j][1])
                dg_ref[pl.ds(blk(c, i, j, h), 8), :] = cell(s_ref, c, i, j, h) - r

    def put(c, i, j, h, value):
        u_ref[pl.ds(blk(c, i, j, h), 8), :] = value

    advance(s_ref, f_ref, sm_ref, None, None, gz_ref, put)


def section_kernel(
    s_ref, slots_ref, ye_ref, yo_ref, xe_ref, xo_ref, gz_ref, dg_ref, first_ref, result_ref,
    u_ref, f_ref, s3_ref, sm_ref, gx_ref, gy_ref, out_ref, slot_ref, sems,
):
    fetch_slot = pltpu.make_async_copy(slots_ref, slot_ref, sems.at[5])
    fetch_slot.start()
    bx, by = row_bit(2), row_bit(1)
    ex, ey = parity("group"), parity("dev")
    for b in range(4):
        for h in range(2):
            for d, g_ref, even_ref, odd_ref, even, bit, step in (
                (0, gx_ref, xe_ref, xo_ref, ex, bx, 2),
                (1, gy_ref, ye_ref, yo_ref, ey, by, 1),
            ):
                first = (0, b) if d == 0 else (b, 0)
                last = (3, b) if d == 0 else (b, 3)
                uf = [cell(s_ref, c, *first, h) for c in range(5)]
                ul = [cell(s_ref, c, *last, h) for c in range(5)]
                he = [even_ref[pl.ds((c * 4 + b) * 8, 8), :] for c in range(5)]
                ho = [odd_ref[pl.ds((c * 4 + b) * 8, 8), :] for c in range(5)]
                hl = [jnp.where(even, ho[c], he[c]) for c in range(5)]
                hh = [jnp.where(even, he[c], ho[c]) for c in range(5)]
                if h == 1:
                    hl = [turn(t, -step) for t in hl]
                    hh = [turn(t, step) for t in hh]
                before = [jnp.where(bit, turn(ul[c], step), hl[c]) for c in range(5)]
                after = [jnp.where(bit, hh[c], turn(uf[c], -step)) for c in range(5)]
                fb, sb = point_flux(before, d)
                fa, sa = point_flux(after, d)
                ff, sf = point_flux(uf, d)
                fl, sl = point_flux(ul, d)
                for c in range(5):
                    at = ((c * 4 + b) * 2 + h) * 8
                    g_ref[pl.ds(at, 8), :] = twice_face(
                        fb[c], ff[c], jnp.maximum(sb, sf), before[c], uf[c]
                    )
                    g_ref[pl.ds(320 + at, 8), :] = twice_face(
                        fl[c], fa[c], jnp.maximum(sa, sl), ul[c], after[c]
                    )

    def put_u(c, i, j, h, value):
        u_ref[pl.ds(blk(c, i, j, h), 8), :] = value

    def put_out(c, i, j, h, value):
        at = pl.ds(blk(c, i, j, h), 8)
        dg = outer_faces(dg_ref[at, :], LIFT, gx_ref, gy_ref, c, i, j, h)
        out_ref[at, :] = jnp.where(troubled, value, dg)

    def store(c):
        rows = pl.ds(c * 256, 256)
        return pltpu.make_async_copy(out_ref.at[rows, :], result_ref.at[rows, :], sems.at[c])

    for c in range(5):
        for i, j in IJ:
            for h in range(2):
                value = first_ref[pl.ds(blk(c, i, j, h), 8), :]
                put_u(c, i, j, h, outer_faces(value, SCALE[0], gx_ref, gy_ref, c, i, j, h))
    nodal(u_ref, f_ref, s3_ref, sm_ref)

    def substep(_, carry):
        advance(u_ref, f_ref, sm_ref, gx_ref, gy_ref, gz_ref, put_u)
        nodal(u_ref, f_ref, s3_ref, sm_ref)
        return carry

    lax.fori_loop(0, SUBSTEPS - 2, substep, 0)
    fetch_slot.wait()
    slot = slot_ref[...]
    troubled = jnp.concatenate([slot, slot], axis=0) >= 0
    advance(
        u_ref, f_ref, sm_ref, gx_ref, gy_ref, gz_ref, put_out, lambda c: store(c).start()
    )
    for c in range(5):
        store(c).wait()


def on_device(state, limit_slot, wall_owner, interpret=False):
    n_group, n_dev = lax.axis_size("group"), lax.axis_size("dev")
    devices = n_group * n_dev
    rows = state.reshape(ROWS, 128)
    halo = jax.ShapeDtypeStruct((160, 128), F32)
    vmem = pl.BlockSpec(memory_space=pltpu.VMEM)
    hbm = pl.BlockSpec(memory_space=pltpu.HBM)
    ye, yo, xe, xo, part = pl.pallas_call(
        prepare_kernel,
        out_shape=(halo, halo, halo, halo, jax.ShapeDtypeStruct((devices, SN_DEV), F32)),
        in_specs=[hbm, hbm],
        out_specs=(vmem,) * 4 + (hbm,),
        scratch_shapes=[
            pltpu.VMEM((ROWS, 128), F32),
            pltpu.SMEM((2, 2, 2), jnp.int32),
            pltpu.VMEM((devices, SN_DEV), F32),
            pltpu.SemaphoreType.DMA((7,)),
        ],
        compiler_params=pltpu.CompilerParams(vmem_limit_bytes=VMEM_LIMIT),
        name="prepare",
        interpret=interpret,
    )(
        pltpu.with_memory_space_constraint(rows, pltpu.HBM),
        pltpu.with_memory_space_constraint(wall_owner, pltpu.HBM),
    )

    def swap(x, axis, odd):
        n = lax.axis_size(axis)
        edges = [(i, (i + 1) % n) for i in range(odd, n, 2)]
        return lax.ppermute(x, axis, edges + [(b, a) for a, b in edges])

    yo = swap(yo, "dev", 1)
    xo = swap(xo, "group", 1)
    ye = swap(ye, "dev", 0)
    xe = swap(xe, "group", 0)
    parts = lax.all_to_all(part, ("group", "dev"), 0, 0, tiled=True)
    wall_loads = pl.pallas_call(
        sum_kernel,
        out_shape=jax.ShapeDtypeStruct((1, SN_DEV), F32),
        in_specs=[vmem],
        out_specs=vmem,
        compiler_params=pltpu.CompilerParams(vmem_limit_bytes=VMEM_LIMIT),
        name="wall_sum",
        interpret=interpret,
    )(parts).reshape(SN_DEV)
    small = pltpu.CompilerParams(vmem_limit_bytes=VMEM_LIMIT)
    volume = pl.pallas_call(
        volume_kernel,
        out_shape=(
            jax.ShapeDtypeStruct((640, 128), F32),
            jax.ShapeDtypeStruct((ROWS, 128), F32),
            jax.ShapeDtypeStruct((ROWS, 128), F32),
        ),
        in_specs=[vmem],
        out_specs=(vmem,) * 3,
        scratch_shapes=[
            pltpu.VMEM((9 * 256, 128), F32),
            pltpu.VMEM((3 * 256, 128), F32),
            pltpu.VMEM((3 * 256, 128), F32),
        ],
        compiler_params=small,
        name="volume",
        interpret=interpret,
    )
    section = pl.pallas_call(
        section_kernel,
        out_shape=jax.ShapeDtypeStruct((ROWS, 128), F32),
        in_specs=[vmem, hbm] + [vmem] * 7,
        out_specs=hbm,
        scratch_shapes=[
            pltpu.VMEM((ROWS, 128), F32),
            pltpu.VMEM((9 * 256, 128), F32),
            pltpu.VMEM((3 * 256, 128), F32),
            pltpu.VMEM((3 * 256, 128), F32),
            pltpu.VMEM((640, 128), F32),
            pltpu.VMEM((640, 128), F32),
            pltpu.VMEM((ROWS, 128), F32),
            pltpu.VMEM((4, 128), jnp.int32),
            pltpu.SemaphoreType.DMA((6,)),
        ],
        compiler_params=small,
        cost_estimate=pl.CostEstimate(flops=60_000_000, transcendentals=600_000, bytes_accessed=2_000_000),
        name="section",
        interpret=interpret,
    )
    gz, dg, first = volume(rows)
    slots = pltpu.with_memory_space_constraint(limit_slot.reshape(4, 128), pltpu.HBM)
    out = section(rows, slots, ye, yo, xe, xo, gz, dg, first)
    return out.reshape(state.shape), wall_loads


def solution(mesh):
    in_specs = (
        P(None, None, None, None, "group", "dev", None),
        P("group", "dev", None),
        P("group", "dev", None),
    )
    out_specs = (P(None, None, None, None, "group", "dev", None), P(("group", "dev")))
    return jax.shard_map(
        on_device, mesh=mesh, in_specs=in_specs, out_specs=out_specs, check_vma=False
    )
```
